128 devices in a mesh: gx: 8 (over z, core), gy: 16 (over x, y).
Axes of the slice: x: 4, y: 4, z: 4, core: 2. Of those that a mesh axis runs over, the one named last changes fastest.
Arguments:
- policy_logp: float32 [16, 2048, 4096], P('gy', 'gx'), may hold values from -2 to 0
- anchor_logp: float32 [16, 2048, 4096], P('gy', 'gx'), may hold values from -2 to 0
- lengths: int32 [16, 2048], P('gy', 'gx'), may hold values from 512 to 4096
- rewards: int32 [16, 2048], P('gy', 'gx'), may hold values from 0 to 8
- slot_prompt: int32 [16, 2048], P('gy', 'gx'), may hold values from 0 to 2047, as said below
Outputs:
- token_grad: float32 [16, 2048, 4096], P(None, ('gx', 'gy'))
- sample_loss: float32 [16, 2048], P(None, ('gx', 'gy'))
- advantage: float32 [16, 2048], P(None, ('gx', 'gy'))
The draws below stay inside these ranges and needn't reach their ends.
Inputs may be any that keep to these rules, and one draw needn't show every extreme that they name: `slot_prompt`: for every member k and every aligned block of 256 slots, the slots of the block hold each prompt of the same block exactly once.
All inputs are finite; a program needn't handle non-finite values.
Results may differ from the reference program's by a relative error of at most 0.00002.
Values sent between devices are 32-bit elements; how exact they have to be, the bound alone decides.
No kernel may reach another device: no remote copies, remote signals or barrier semaphores. Data moves between devices by JAX's collectives and lax.ppermute only.
A program may use at most 64 MiB of HBM per device.

```python
import jax
import jax.numpy as jnp

K = 16
LMAX = 4096
PROMPTS = 2048
BLOCK = 256
SAMPLES = 32768
N_GX = 8


def draw_slot_prompt(key, part):
    subkeys = jax.random.split(jax.random.fold_in(key, 7), K * N_GX)
    shuffled = jax.vmap(lambda subkey: jax.random.permutation(subkey, BLOCK))(subkeys)
    shuffled = shuffled.astype(jnp.int32).reshape(K, N_GX, BLOCK)
    offsets = (jnp.arange(N_GX, dtype=jnp.int32) * BLOCK)[None, :, None]
    return (shuffled + offsets).reshape(K, PROMPTS).astype(jnp.int32)


def with_ends(values, stream_key, least, high):
    spot = [jax.random.randint(jax.random.fold_in(stream_key, axis), (), 0, length) for axis, length in enumerate(values.shape)]
    widest = values.shape.index(max(values.shape))
    neighbour = spot[:widest] + [(spot[widest] + 1) % values.shape[widest]] + spot[widest + 1:]
    return values.at[tuple(spot)].set(least).at[tuple(neighbour)].set(high)


def level_of(stream_key, shape, cuts, low, top_value):
    level, own = 1.0, jax.random.fold_in(stream_key, 6)
    for dim, shards_of in cuts:
        steps = jnp.exp(jax.random.uniform(jax.random.fold_in(own, dim), (shards_of,), jnp.float32, low / len(cuts), top_value / len(cuts)))
        level = level * jnp.repeat(steps, shape[dim] // shards_of).reshape([-1 if axis == dim else 1 for axis in range(len(shape))])
    return level


def setup_inputs(seed: int = 0) -> dict:
    key_list = jax.random.split(jax.random.key(seed), 6)
    policy_logp = jnp.clip(-2.0 + 2.0 * jax.random.uniform(key_list[0], (K, PROMPTS, LMAX), jnp.float32) ** level_of(key_list[0], (K, PROMPTS, LMAX), ((0, 16), (1, 8)), -0.2, 0.2), -2.0, 0.0)
    anchor_logp = jnp.clip(-2.0 + 2.0 * jax.random.uniform(key_list[1], (K, PROMPTS, LMAX), jnp.float32) ** level_of(key_list[1], (K, PROMPTS, LMAX), ((0, 16), (1, 8)), -0.2, 0.2), -2.0, 0.0)
    lengths = with_ends(jax.random.randint(key_list[2], (K, PROMPTS), LMAX // 8, LMAX + 1), jax.random.fold_in(key_list[2], 1), LMAX // 8, LMAX).astype(jnp.int32)
    rewards = with_ends(jax.random.randint(key_list[3], (K, PROMPTS), 0, 9), jax.random.fold_in(key_list[3], 1), 0, 8).astype(jnp.int32)
    slot_prompt = draw_slot_prompt(jax.random.fold_in(key_list[5], 71), 0)
    return dict(policy_logp=policy_logp, anchor_logp=anchor_logp, lengths=lengths, rewards=rewards, slot_prompt=slot_prompt)


kl_weight = 0.1


def reference(policy_logp, anchor_logp, lengths, rewards, slot_prompt):
    member_rows = jnp.arange(K, dtype=jnp.int32)[:, None]
    slot_ids = jnp.broadcast_to(jnp.arange(PROMPTS, dtype=jnp.int32)[None, :], (K, PROMPTS))
    inverse = jnp.zeros((K, PROMPTS), jnp.int32).at[member_rows, slot_prompt].set(slot_ids)
    policy = jnp.take_along_axis(policy_logp, inverse[:, :, None], axis=1)
    anchor = jnp.take_along_axis(anchor_logp, inverse[:, :, None], axis=1)
    seq_len = jnp.take_along_axis(lengths, inverse, axis=1)
    reward = jnp.take_along_axis(rewards, inverse, axis=1).astype(jnp.float32) * 0.25
    total = jnp.sum(reward, axis=0)
    advantage = (K * reward - total[None, :]) / (K - 1)
    ntok = jnp.sum(lengths).astype(jnp.float32)
    positions = jnp.arange(LMAX, dtype=jnp.int32)[None, None, :]
    valid = positions < seq_len[:, :, None]
    log_ratio = anchor - policy
    ratio = jnp.exp(log_ratio)
    token_term = -advantage[:, :, None] * policy + kl_weight * (ratio - log_ratio - 1.0)
    token_grad = jnp.where(valid, -advantage[:, :, None] + kl_weight * (1.0 - ratio), 0.0) * (SAMPLES * LMAX / ntok)
    sample_loss = jnp.sum(jnp.where(valid, token_term, 0.0), axis=2) * (SAMPLES / ntok)
    return token_grad, sample_loss, advantage
```

```python
import jax
import jax.numpy as jnp
from jax import lax
from jax.experimental import pallas as pl
from jax.experimental.pallas import tpu as pltpu
from jax.sharding import Mesh
from jax.sharding import PartitionSpec as P

GX_GY = ("gx_0", "gx_1", "gy_0", "gy_1")
GY = ("gy_0", "gy_1")
GX = ("gx_0", "gx_1")

KL = 0.1
LANES = 128
META = 8
FAST = 432


def lane_rows(x, rows, width):
    return (
        x.reshape(rows // 8, 8, width // LANES, LANES)
        .transpose(0, 2, 1, 3)
        .reshape(rows * width // LANES, LANES)
    )


def pack_kernel(
    dests,
    per_dest,
    cols,
    len_ref,
    prompt_ref,
    vec_ref,
    tok_ref,
    policy_hbm,
    anchor_hbm,
    main_hbm,
    rest_hbm,
    policy,
    anchor,
    stage,
    part_p,
    part_q,
    meta,
    len_of,
    slot_of,
    in_sem,
    out_sem,
):
    slots = dests * per_dest
    full = META + per_dest * cols
    head = META + FAST
    loads = [
        pltpu.make_async_copy(policy_hbm, policy, in_sem.at[0]),
        pltpu.make_async_copy(anchor_hbm, anchor, in_sem.at[1]),
    ]
    for load in loads:
        load.start()

    @pl.loop(0, slots)
    def _(s):
        p = lax.rem(prompt_ref[0, s], slots)
        len_of[p] = len_ref[0, s]
        slot_of[p] = s

    ids = lax.broadcasted_iota(jnp.int32, (slots, slots), 0)
    pick = jnp.where(lax.rem(vec_ref[2:3, :], slots) == ids, 1.0, 0.0)
    values = vec_ref[0:8, :].astype(jnp.float32)
    ordered = lax.dot_general(
        values,
        pick,
        (((1,), (1,)), ((), ())),
        precision=lax.Precision.HIGHEST,
        preferred_element_type=jnp.float32,
    )
    position = lax.broadcasted_iota(jnp.int32, (cols, LANES), 0) * LANES + lax.broadcasted_iota(
        jnp.int32, (cols, LANES), 1
    )
    for load in loads:
        load.wait()

    def out_copies(dest, slot):
        return (
            pltpu.make_async_copy(
                stage.at[slot, pl.ds(0, head)], main_hbm.at[dest], out_sem.at[0, slot]
            ),
            pltpu.make_async_copy(
                stage.at[slot, pl.ds(head, full - head)], rest_hbm.at[dest], out_sem.at[1, slot]
            ),
        )

    for dest in range(dests):

        def row(r, carry):
            at, dest = carry
            p = dest * per_dest + r
            s = slot_of[p]
            length = len_of[p]
            first = lax.div(s, 8) * (8 * cols) + lax.rem(s, 8)
            a = policy[pl.ds(first, cols, stride=8), :]
            d = anchor[pl.ds(first, cols, stride=8), :] - a
            e = jnp.exp(d)
            valid = position < length
            stage[dest, pl.ds(at, cols), :] = jnp.where(valid, KL * (1.0 - e), 0.0)
            term_p = jnp.where(valid, a, 0.0)
            term_q = jnp.where(valid, KL * (e - d - 1.0), 0.0)
            part_p[p, :, :] = jnp.sum(term_p.reshape(cols // 8, 8, LANES), axis=0)
            part_q[p, :, :] = jnp.sum(term_q.reshape(cols // 8, 8, LANES), axis=0)
            return at + lax.div(length + (LANES - 1), LANES), dest

        lax.fori_loop(0, per_dest, row, (META, dest), unroll=4)

    ones = jnp.full((8, LANES), 1.0, jnp.float32)

    def lanes(part):
        return lax.dot_general(
            ones,
            jnp.sum(part[...], axis=1),
            (((1,), (1,)), ((), ())),
            precision=lax.Precision.HIGHEST,
            preferred_element_type=jnp.float32,
        )[0:1]

    rows_of = jnp.floor((ordered[0:1] + (LANES - 1.0)) * (1.0 / LANES))
    sums_p, sums_q = lanes(part_p), lanes(part_q)
    tokens = jnp.full((1, LANES), 1.0, jnp.float32) * tok_ref[0, 0]
    meta[4:5, :] = tokens
    group = lax.broadcasted_iota(jnp.int32, (1, slots), 1)
    most = jnp.zeros((1, 1), jnp.float32)
    for dest in range(dests):
        inside = (group >= dest * per_dest) & (group < (dest + 1) * per_dest)
        most = jnp.maximum(most, jnp.sum(jnp.where(inside, rows_of, 0.0), axis=1, keepdims=True))
    for dest in range(dests):
        half = dest * per_dest // LANES * LANES
        stage[dest, 0:1, :] = ordered[0:1, half : half + LANES]
        stage[dest, 1:2, :] = ordered[1:2, half : half + LANES]
        stage[dest, 2:3, :] = sums_p[:, half : half + LANES]
        stage[dest, 3:4, :] = sums_q[:, half : half + LANES]
        stage[dest, 4:5, :] = tokens
        stage[dest, 5:8, :] = jnp.broadcast_to(most, (3, LANES))
        for copy in out_copies(dest, dest):
            copy.start()
    for dest in range(dests):
        for copy in out_copies(dest, dest):
            copy.wait()


def pack(lengths, prompts, vec, tokens, policy, anchor, dests):
    slots = lengths.shape[1]
    per_dest = slots // dests
    cols = policy.shape[0] // slots
    full = META + per_dest * cols
    head = META + FAST
    smem = pl.BlockSpec(memory_space=pltpu.SMEM)
    hbm = pl.BlockSpec(memory_space=pl.ANY)

    def body(*refs):
        pack_kernel(dests, per_dest, cols, *refs)

    return pl.pallas_call(
        body,
        out_shape=(
            jax.ShapeDtypeStruct((dests, head, LANES), jnp.float32),
            jax.ShapeDtypeStruct((dests, full - head, LANES), jnp.float32),
        ),
        in_specs=[smem, smem, pl.BlockSpec(memory_space=pltpu.VMEM), smem, hbm, hbm],
        out_specs=(hbm, hbm),
        scratch_shapes=[
            pltpu.VMEM((slots * cols, LANES), jnp.float32),
            pltpu.VMEM((slots * cols, LANES), jnp.float32),
            pltpu.VMEM((dests, full + cols, LANES), jnp.float32),
            pltpu.VMEM((slots, 8, LANES), jnp.float32),
            pltpu.VMEM((slots, 8, LANES), jnp.float32),
            pltpu.VMEM((8, LANES), jnp.float32),
            pltpu.SMEM((slots,), jnp.int32),
            pltpu.SMEM((slots,), jnp.int32),
            pltpu.SemaphoreType.DMA((2,)),
            pltpu.SemaphoreType.DMA((2, dests)),
        ],
        name="pack",
    )(lengths, prompts, vec, tokens, policy, anchor)


def score_kernel(
    members,
    per_dest,
    cols,
    scales,
    parts,
    refs,
):
    (
        *got_hbm,
        grad_hbm,
        loss_ref,
        adv_ref,
        got,
        grad,
        meta,
        numbers,
        rows_at,
        got_sem,
        num_sem,
        out_sem,
    ) = refs
    grad_scale, loss_scale = scales
    width = per_dest * cols

    def in_copies(k):
        at, copies = 0, []
        for i, (part, size) in enumerate(zip(got_hbm, parts)):
            copies.append(
                pltpu.make_async_copy(part.at[k], got.at[k, pl.ds(at, size)], got_sem.at[i, k])
            )
            at += size
        return copies

    heads = [
        pltpu.make_async_copy(got_hbm[0].at[k, pl.ds(0, META)], meta.at[k], num_sem.at[k])
        for k in range(members)
    ]
    for copy in heads:
        copy.start()
    for k in range(members):
        for copy in in_copies(k):
            copy.start()
    for copy in heads:
        copy.wait()

    def field(i):
        return jnp.concatenate([meta[k, i : i + 1, :] for k in range(members)], axis=0)

    reward = field(1) * 0.25
    total = jnp.sum(reward, axis=0, keepdims=True)
    advantage = (members * reward - total) / (members - 1)
    tokens = jnp.sum(field(4), axis=0, keepdims=True)
    loss = (field(3) - advantage * field(2)) * (loss_scale / tokens)
    mine = lax.axis_index(GY)
    start = lax.rem(mine * per_dest, LANES)
    shift = lax.rem(LANES - start, LANES)
    loss_ref[...] = pltpu.roll(loss, shift, 1)[:, 0:per_dest]
    adv_ref[...] = pltpu.roll(advantage, shift, 1)[:, 0:per_dest]
    rows_at[0] = pltpu.roll(field(0), shift, 1)
    rows_at[1] = pltpu.roll(advantage, shift, 1)
    rows_at[2] = jnp.broadcast_to(grad_scale / tokens, (members, LANES))
    to_scalars = pltpu.make_async_copy(rows_at, numbers, num_sem.at[members])
    to_scalars.start()
    to_scalars.wait()
    scale = numbers[2, 0, 0]
    position = lax.broadcasted_iota(jnp.int32, (cols, LANES), 0) * LANES + lax.broadcasted_iota(
        jnp.int32, (cols, LANES), 1
    )

    def out_copy(k):
        return pltpu.make_async_copy(
            grad.at[pl.ds(k * width, width)], grad_hbm.at[pl.ds(k * width, width)], out_sem.at[k]
        )

    @pl.loop(0, members)
    def _(k):
        for copy in in_copies(k):
            copy.wait()

        def row(r, at):
            length = numbers[0, k, r].astype(jnp.int32)
            x = got[k, pl.ds(at, cols), :]
            y = jnp.where(position < length, x - numbers[1, k, r], 0.0) * scale
            first = k * width + lax.div(r, 8) * (8 * cols) + lax.rem(r, 8)
            grad[pl.ds(first, cols, stride=8), :] = y
            return at + lax.div(length + (LANES - 1), LANES)

        lax.fori_loop(0, per_dest, row, META, unroll=4)
        out_copy(k).start()

    @pl.loop(0, members)
    def _(k):
        out_copy(k).wait()


def score(got, scales, per_dest, cols):
    members = got[0].shape[0]
    parts = [g.shape[1] for g in got]
    full = META + per_dest * cols
    hbm = pl.BlockSpec(memory_space=pl.ANY)
    vmem = pl.BlockSpec(memory_space=pltpu.VMEM)

    def body(*refs):
        score_kernel(members, per_dest, cols, scales, parts, refs)

    small = jax.ShapeDtypeStruct((members, per_dest), jnp.float32)
    return pl.pallas_call(
        body,
        out_shape=(
            jax.ShapeDtypeStruct((members * per_dest * cols, LANES), jnp.float32),
            small,
            small,
        ),
        in_specs=[hbm] * len(got),
        out_specs=(hbm, vmem, vmem),
        scratch_shapes=[
            pltpu.VMEM((members, full + cols, LANES), jnp.float32),
            pltpu.VMEM((members * per_dest * cols, LANES), jnp.float32),
            pltpu.VMEM((members, META, LANES), jnp.float32),
            pltpu.SMEM((3, members, LANES), jnp.float32),
            pltpu.VMEM((3, members, LANES), jnp.float32),
            pltpu.SemaphoreType.DMA((len(got), members)),
            pltpu.SemaphoreType.DMA((members + 1,)),
            pltpu.SemaphoreType.DMA((members,)),
        ],
        name="score",
    )(*got)


def over_gx(x):
    for axis, size in (("gx_0", lax.axis_size("gx_0")), ("gx_1", lax.axis_size("gx_1"))):
        step = 1
        while step < size:
            x = x + lax.ppermute(x, axis, [(i, i ^ step) for i in range(size)])
            step *= 2
    return x


def body(policy_logp, anchor_logp, lengths, rewards, slot_prompt):
    members_dev, slots, seq_slots = policy_logp.shape
    dests = lax.axis_size(GY)
    per_dest = slots // dests
    cols = seq_slots // LANES
    members = members_dev * dests
    samples = members * slots * lax.axis_size(GX)
    scales = (float(samples * seq_slots), float(samples))
    tokens = over_gx(jnp.sum(lengths.astype(jnp.float32)).reshape(1, 1))
    vec = jnp.concatenate([lengths, rewards, slot_prompt] + [slot_prompt] * 5, axis=0)
    main, rest = pack(
        lengths,
        slot_prompt,
        vec,
        tokens,
        lane_rows(policy_logp, slots, seq_slots),
        lane_rows(anchor_logp, slots, seq_slots),
        dests,
    )
    main = lax.all_to_all(main, GY, 0, 0, tiled=True)
    most = jnp.max(main[:, 5, 0])

    def all_there(main, rest):
        return score((main,), scales, per_dest, cols)

    def more_to_come(main, rest):
        rest = lax.all_to_all(rest, GY, 0, 0, tiled=True)
        return score((main, rest), scales, per_dest, cols)

    grad, loss, advantage = lax.cond(most <= FAST, all_there, more_to_come, main, rest)
    grad = (
        grad.reshape(members, per_dest // 8, cols, 8, LANES)
        .transpose(0, 1, 3, 2, 4)
        .reshape(members, per_dest, seq_slots)
    )
    return grad, loss, advantage


def solution(mesh):
    torus = Mesh(mesh.devices.reshape(4, 2, 4, 4), ("gx_0", "gx_1", "gy_0", "gy_1"))
    return jax.shard_map(
        body,
        mesh=torus,
        in_specs=(P(GY, GX, None), P(GY, GX, None), P(GY, GX), P(GY, GX), P(GY, GX)),
        out_specs=(P(None, GX_GY, None), P(None, GX_GY), P(None, GX_GY)),
        check_vma=False,
    )
```

```python
import jax
import jax.numpy as jnp
from jax import lax
from jax.experimental import pallas as pl
from jax.experimental.pallas import tpu as pltpu
from jax.sharding import Mesh
from jax.sharding import PartitionSpec as P

GX_GY = ("gx_0", "gx_1", "gy_0", "gy_1")
GY = ("gy_0", "gy_1")
GX = ("gx_0", "gx_1")

KL = 0.1
LANES = 128
META = 8
FAST = 432


def lane_rows(x, rows, width):
    return (
        x.reshape(rows // 8, 8, width // LANES, LANES)
        .transpose(0, 2, 1, 3)
        .reshape(rows * width // LANES, LANES)
    )


def sliced_position(cols):
    row = lax.broadcasted_iota(jnp.int32, (cols, LANES), 0)
    return row * LANES + lax.broadcasted_iota(jnp.int32, (cols, LANES), 1)


STEPS = 8


def token_kernel(len_ref, policy_hbm, anchor_hbm, u_ref, p_ref, q_ref, policy, anchor, sem):
    slots, width = policy.shape
    rows = slots // STEPS

    def loads(step):
        part = pl.ds(pl.multiple_of(step * rows, rows), rows)
        return (
            pltpu.make_async_copy(policy_hbm.at[part], policy.at[part], sem.at[0, step]),
            pltpu.make_async_copy(anchor_hbm.at[part], anchor.at[part], sem.at[1, step]),
        )

    for step in range(STEPS):
        for load in loads(step):
            load.start()
    lane = lax.broadcasted_iota(jnp.int32, (8, LANES), 1)
    sub = lax.broadcasted_iota(jnp.int32, (8, LANES), 0)

    @pl.loop(0, STEPS)
    def _(step):
        for load in loads(step):
            load.wait()

        @pl.loop(0, rows // 8)
        def _(group):
            first = pl.multiple_of(step * rows + group * 8, 8)
            length = jnp.full((8, LANES), len_ref[0, first], jnp.int32)
            for i in range(1, 8):
                length = jnp.where(sub == i, len_ref[0, first + i], length)
            behind = lane - length
            sums_p = [jnp.zeros((8, LANES), jnp.float32)] * 4
            sums_q = [jnp.zeros((8, LANES), jnp.float32)] * 4
            for c in range(width // LANES):
                at = (pl.ds(first, 8), pl.ds(c * LANES, LANES))
                a = policy[at]
                d = anchor[at] - a
                valid = behind < -c * LANES
                u = jnp.where(valid, jnp.exp(d) - 1.0, 0.0)
                u_ref[at] = u
                sums_q[c % 4] = sums_q[c % 4] + (u - jnp.where(valid, d, 0.0))
                sums_p[c % 4] = sums_p[c % 4] + jnp.where(valid, a, 0.0)
            p_ref[pl.ds(first, 8), :] = (sums_p[0] + sums_p[1]) + (sums_p[2] + sums_p[3])
            q_ref[pl.ds(first, 8), :] = (sums_q[0] + sums_q[1]) + (sums_q[2] + sums_q[3])


def token_terms(lengths, policy, anchor):
    slots, width = policy.shape
    vmem = pl.BlockSpec(memory_space=pltpu.VMEM)
    hbm = pl.BlockSpec(memory_space=pltpu.HBM)
    small = jax.ShapeDtypeStruct((slots, LANES), jnp.float32)
    return pl.pallas_call(
        token_kernel,
        out_shape=(jax.ShapeDtypeStruct((slots, width), jnp.float32), small, small),
        in_specs=[pl.BlockSpec(memory_space=pltpu.SMEM), hbm, hbm],
        out_specs=(vmem, vmem, vmem),
        scratch_shapes=[
            pltpu.VMEM((slots, width), jnp.float32),
            pltpu.VMEM((slots, width), jnp.float32),
            pltpu.SemaphoreType.DMA((2, STEPS)),
        ],
        compiler_params=pltpu.CompilerParams(vmem_limit_bytes=24 << 20),
        cost_estimate=pl.CostEstimate(
            flops=40_000_000, bytes_accessed=12 * slots * width, transcendentals=slots * width
        ),
        name="token_terms",
    )(lengths, policy, anchor)


def pack_kernel(
    dests,
    per_dest,
    cols,
    len_ref,
    reward_ref,
    prompt_ref,
    tok_refs,
    u_ref,
    p_ref,
    q_ref,
    main,
    stage,
    sorted_p,
    sorted_q,
    slot_of,
):
    slots = dests * per_dest
    chunk = META + FAST

    def invert(s, carry):
        slot_of[prompt_ref[0, s] & (slots - 1)] = s
        return carry

    lax.fori_loop(0, slots, invert, 0, unroll=16)
    lane = lax.broadcasted_iota(jnp.int32, (8, LANES), 1)
    sub = lax.broadcasted_iota(jnp.int32, (8, LANES), 0)

    def one_dest(dest, most, ref, base):
        at = base + META
        meta = jnp.zeros((8, LANES), jnp.float32)
        for r in range(per_dest):
            p = dest * per_dest + r
            s = slot_of[p]
            length = len_ref[0, s]
            first = (s >> 3) * (8 * cols) + (s & 7)
            ref[pl.ds(at, cols), :] = u_ref[pl.ds(first, cols, stride=8), :]
            sorted_p[pl.ds(p, 1), :] = p_ref[pl.ds(s, 1), :]
            sorted_q[pl.ds(p, 1), :] = q_ref[pl.ds(s, 1), :]
            both = jnp.where(
                sub == 0,
                length.astype(jnp.float32),
                reward_ref[0, s].astype(jnp.float32) * 0.25,
            )
            meta = jnp.where(lane == r, both, meta)
            at = at + ((length + (LANES - 1)) >> 7)
        ref[pl.ds(base, META), :] = meta
        return jnp.maximum(most, at - base - META)

    last = dests - 1

    def in_place(dest, most):
        return one_dest(dest, most, main, pl.multiple_of(dest * chunk, 8))

    most = lax.fori_loop(0, last, in_place, jnp.int32(0))
    most = one_dest(last, most, stage, 0)
    main[last * chunk : (last + 1) * chunk, :] = stage[0:chunk, :]

    ones = jnp.full((8, LANES), 1.0, jnp.float32)

    def lanes(part):
        return lax.dot_general(
            ones,
            part[...],
            (((1,), (1,)), ((), ())),
            precision=lax.Precision.HIGHEST,
            preferred_element_type=jnp.float32,
        )

    sums_p, sums_q = lanes(sorted_p), lanes(sorted_q)
    tokens = jnp.sum(sum(t[...] for t in tok_refs).astype(jnp.float32), axis=1, keepdims=True)
    fill = most.astype(jnp.float32)
    for dest in range(dests):
        half = dest * per_dest // LANES * LANES
        head = slice(dest * chunk, dest * chunk + META)
        rows = jnp.where(sub == 2, sums_p[:, half : half + LANES], main[head, :])
        rows = jnp.where(sub == 3, sums_q[:, half : half + LANES], rows)
        rows = jnp.where(sub == 4, tokens, rows)
        main[head, :] = jnp.where(sub == 5, fill, rows)


def pack(lengths, rewards, prompts, tokens, u, sums_p, sums_q, dests):
    slots = lengths.shape[1]
    per_dest = slots // dests
    cols = u.shape[0] // slots
    chunk = META + FAST
    smem = pl.BlockSpec(memory_space=pltpu.SMEM)
    vmem = pl.BlockSpec(memory_space=pltpu.VMEM)

    def body(*refs):
        mine, refs = refs[:3], refs[3:]
        tok_refs, refs = refs[: len(tokens)], refs[len(tokens) :]
        pack_kernel(dests, per_dest, cols, *mine, tok_refs, *refs)

    return pl.pallas_call(
        body,
        out_shape=jax.ShapeDtypeStruct((dests * chunk, LANES), jnp.float32),
        in_specs=[smem] * 3 + [vmem] * (len(tokens) + 3),
        out_specs=vmem,
        scratch_shapes=[
            pltpu.VMEM((META + (per_dest + 1) * cols, LANES), jnp.float32),
            pltpu.VMEM((slots, LANES), jnp.float32),
            pltpu.VMEM((slots, LANES), jnp.float32),
            pltpu.SMEM((slots,), jnp.int32),
        ],
        compiler_params=pltpu.CompilerParams(vmem_limit_bytes=24 << 20),
        name="pack",
    )(lengths, rewards, prompts, *tokens, u, sums_p, sums_q).reshape(dests, chunk, LANES)


def pack_rest(lengths, prompts, u, dests):
    slots = lengths.shape[1]
    per_dest = slots // dests
    cols = u.shape[0] // slots
    spare = per_dest * cols - FAST

    def body(len_ref, prompt_ref, u_ref, rest_hbm, stage, slot_of, sem):
        def invert(s, carry):
            slot_of[prompt_ref[0, s] & (slots - 1)] = s
            return carry

        lax.fori_loop(0, slots, invert, 0)

        def one_dest(dest, carry):
            def row(r, at):
                s = slot_of[dest * per_dest + r]
                first = (s >> 3) * (8 * cols) + (s & 7)
                stage[pl.ds(at, cols), :] = u_ref[pl.ds(first, cols, stride=8), :]
                return at + ((len_ref[0, s] + (LANES - 1)) >> 7)

            lax.fori_loop(0, per_dest, row, jnp.int32(0))
            copy = pltpu.make_async_copy(stage.at[pl.ds(FAST, spare)], rest_hbm.at[dest], sem)
            copy.start()
            copy.wait()
            return carry

        lax.fori_loop(0, dests, one_dest, 0)

    smem = pl.BlockSpec(memory_space=pltpu.SMEM)
    return pl.pallas_call(
        body,
        out_shape=jax.ShapeDtypeStruct((dests, spare, LANES), jnp.float32),
        in_specs=[smem, smem, pl.BlockSpec(memory_space=pltpu.VMEM)],
        out_specs=pl.BlockSpec(memory_space=pl.ANY),
        scratch_shapes=[
            pltpu.VMEM(((per_dest + 1) * cols, LANES), jnp.float32),
            pltpu.SMEM((slots,), jnp.int32),
            pltpu.SemaphoreType.DMA,
        ],
        compiler_params=pltpu.CompilerParams(vmem_limit_bytes=16 << 20),
        name="pack_rest",
    )(lengths, prompts, u)


def score_kernel(members, per_dest, cols, scales, refs):
    main, grad_hbm, loss_ref, adv_ref, table_ref, more_ref, tail, grad, numbers, num_sem, out_sem = refs
    grad_scale, loss_scale = scales
    width = per_dest * cols
    chunk = META + FAST

    def field(i):
        return jnp.concatenate(
            [main[k * chunk + i : k * chunk + i + 1, :] for k in range(members)], axis=0
        )

    reward = field(1)
    total = jnp.sum(reward, axis=0, keepdims=True)
    advantage = (members * reward - total) / (members - 1)
    tokens = jnp.sum(field(4), axis=0, keepdims=True)
    scale = grad_scale / tokens
    table_ref[0] = field(0)
    table_ref[1] = -advantage * scale
    table_ref[2] = jnp.broadcast_to(scale * -KL, (members, LANES))
    to_scalars = pltpu.make_async_copy(table_ref, numbers, num_sem)
    to_scalars.start()

    start = lax.rem(lax.axis_index(GY) * per_dest, LANES)
    shift = lax.rem(LANES - start, LANES)
    sums_p = pltpu.roll(field(2), shift, 1)
    sums_q = pltpu.roll(field(3), shift, 1)
    loss = (KL * sums_q - advantage * sums_p) * (loss_scale / tokens)
    loss_ref[...] = loss[:, 0:per_dest]
    adv_ref[...] = advantage[:, 0:per_dest]
    most = jnp.max(field(5), axis=0, keepdims=True)
    more_ref[...] = jnp.where(most > FAST, 1, 0)
    position = sliced_position(cols)
    last = members - 1
    tail[0:chunk, :] = main[last * chunk : (last + 1) * chunk, :]
    to_scalars.wait()

    def out_copy(k):
        part = pl.ds(pl.multiple_of(k * width, width), width)
        return pltpu.make_async_copy(grad.at[part], grad_hbm.at[part], out_sem.at[k])

    def one_member(k, ref, base):
        slope = numbers[2, 0, 0]
        at = base + META
        for r in range(per_dest):
            length = numbers[0, k, r].astype(jnp.int32)
            u = ref[pl.ds(at, cols), :]
            y = jnp.where(position < length, numbers[1, k, r] + slope * u, 0.0)
            first = k * width + r // 8 * (8 * cols) + r % 8
            grad[pl.ds(first, cols, stride=8), :] = y
            at = jnp.minimum(at + ((length + (LANES - 1)) >> 7), base + chunk)
        out_copy(k).start()

    @pl.loop(0, last)
    def _(k):
        one_member(k, main, pl.multiple_of(k * chunk, 8))

    one_member(last, tail, 0)

    @pl.loop(0, members)
    def _(k):
        out_copy(k).wait()


def score(main, scales, per_dest, cols):
    members, chunk, _ = main.shape
    full = per_dest * cols
    hbm = pl.BlockSpec(memory_space=pl.ANY)
    vmem = pl.BlockSpec(memory_space=pltpu.VMEM)

    def body(*refs):
        score_kernel(members, per_dest, cols, scales, refs)

    small = jax.ShapeDtypeStruct((members, per_dest), jnp.float32)
    return pl.pallas_call(
        body,
        out_shape=(
            jax.ShapeDtypeStruct((members * full, LANES), jnp.float32),
            small,
            small,
            jax.ShapeDtypeStruct((3, members, LANES), jnp.float32),
            jax.ShapeDtypeStruct((1, LANES), jnp.int32),
        ),
        in_specs=[vmem],
        out_specs=(hbm, vmem, vmem, vmem, vmem),
        scratch_shapes=[
            pltpu.VMEM((chunk + cols, LANES), jnp.float32),
            pltpu.VMEM((members * full, LANES), jnp.float32),
            pltpu.SMEM((3, members, LANES), jnp.float32),
            pltpu.SemaphoreType.DMA,
            pltpu.SemaphoreType.DMA((members,)),
        ],
        compiler_params=pltpu.CompilerParams(vmem_limit_bytes=24 << 20),
        name="score",
    )(main.reshape(members * chunk, LANES))


def finish_kernel(members, per_dest, cols, refs):
    table_hbm, rest_hbm, _, grad_hbm, numbers, rest, grad, sem = refs
    width = per_dest * cols
    spare = width - FAST
    load = pltpu.make_async_copy(table_hbm, numbers, sem.at[0])
    load.start()
    load.wait()
    position = sliced_position(cols)
    row_of = lax.broadcasted_iota(jnp.int32, (cols, LANES), 0)

    @pl.loop(0, members)
    def _(k):
        place = grad_hbm.at[pl.ds(k * width, width)]
        loads = (
            pltpu.make_async_copy(rest_hbm.at[k], rest.at[pl.ds(cols, spare)], sem.at[0]),
            pltpu.make_async_copy(place, grad, sem.at[1]),
        )
        for load in loads:
            load.start()
        for load in loads:
            load.wait()

        def row(r, at):
            length = numbers[0, k, r].astype(jnp.int32)
            end = at + ((length + (LANES - 1)) >> 7)

            @pl.when(end > FAST)
            def _():
                u = rest[pl.ds(at - FAST + cols, cols), :]
                y = jnp.where(position < length, numbers[1, k, r] + numbers[2, 0, 0] * u, 0.0)
                first = (r >> 3) * (8 * cols) + (r & 7)
                old = grad[pl.ds(first, cols, stride=8), :]
                grad[pl.ds(first, cols, stride=8), :] = jnp.where(row_of + at >= FAST, y, old)

            return end

        lax.fori_loop(0, per_dest, row, jnp.int32(0))
        store = pltpu.make_async_copy(grad, place, sem.at[1])
        store.start()
        store.wait()


def finish(grad, rest, table, per_dest, cols):
    members = rest.shape[0]
    full = per_dest * cols
    hbm = pl.BlockSpec(memory_space=pl.ANY)

    def body(*refs):
        finish_kernel(members, per_dest, cols, refs)

    return pl.pallas_call(
        body,
        out_shape=jax.ShapeDtypeStruct(grad.shape, jnp.float32),
        in_specs=[hbm, hbm, hbm],
        out_specs=hbm,
        input_output_aliases={2: 0},
        scratch_shapes=[
            pltpu.SMEM((3, members, LANES), jnp.float32),
            pltpu.VMEM((full - FAST + 2 * cols, LANES), jnp.float32),
            pltpu.VMEM((full, LANES), jnp.float32),
            pltpu.SemaphoreType.DMA((2,)),
        ],
        compiler_params=pltpu.CompilerParams(vmem_limit_bytes=8 << 20),
        name="finish",
    )(table, rest, grad)


def peers(x, axis):
    size = lax.axis_size(axis)
    return [
        lax.ppermute(x, axis, [(i, (i + step) % size) for i in range(size)])
        for step in range(1, size)
    ]


def body(policy_logp, anchor_logp, lengths, rewards, slot_prompt):
    members_dev, slots, seq_slots = policy_logp.shape
    dests = lax.axis_size(GY)
    per_dest = slots // dests
    cols = seq_slots // LANES
    members = members_dev * dests
    samples = members * slots * lax.axis_size(GX)
    scales = (float(samples * seq_slots), float(samples))
    tokens = [lengths] + peers(lengths, GX)
    u, sums_p, sums_q = token_terms(
        lengths,
        pltpu.with_memory_space_constraint(policy_logp[0], pltpu.HBM),
        pltpu.with_memory_space_constraint(anchor_logp[0], pltpu.HBM),
    )
    u = lane_rows(u, slots, seq_slots)
    main = pack(lengths, rewards, slot_prompt, tokens, u, sums_p, sums_q, dests)
    main = lax.all_to_all(main, GY, 0, 0, tiled=True)
    grad, loss, advantage, table, more = score(main, scales, per_dest, cols)

    def the_rest(state):
        grad, _ = state
        rest = pack_rest(lengths, slot_prompt, u, dests)
        got = lax.all_to_all(rest, GY, 0, 0, tiled=True)
        return finish(grad, got, table, per_dest, cols), jnp.int32(0)

    grad, _ = lax.while_loop(lambda state: state[1] > 0, the_rest, (grad, more[0, 0]))
    grad = (
        grad.reshape(members, per_dest // 8, cols, 8, LANES)
        .transpose(0, 1, 3, 2, 4)
        .reshape(members, per_dest, seq_slots)
    )
    return grad, loss, advantage


def solution(mesh):
    torus = Mesh(mesh.devices.reshape(4, 2, 4, 4), ("gx_0", "gx_1", "gy_0", "gy_1"))
    return jax.shard_map(
        body,
        mesh=torus,
        in_specs=(P(GY, GX, None), P(GY, GX, None), P(GY, GX), P(GY, GX), P(GY, GX)),
        out_specs=(P(None, GX_GY, None), P(None, GX_GY), P(None, GX_GY)),
        check_vma=False,
    )
```

```python
import jax
import jax.numpy as jnp
from jax import lax
from jax.experimental import pallas as pl
from jax.experimental.pallas import tpu as pltpu
from jax.sharding import Mesh
from jax.sharding import PartitionSpec as P

GX_GY = ("gx_0", "gx_1", "gy_0", "gy_1")
GY = ("gy_0", "gy_1")
GX = ("gx_0", "gx_1")

KL = 0.1
LANES = 128
META = 8
FAST = 432


def lane_rows(x, rows, width):
    return (
        x.reshape(rows // 8, 8, width // LANES, LANES)
        .transpose(0, 2, 1, 3)
        .reshape(rows * width // LANES, LANES)
    )


def sliced_position(cols):
    row = lax.broadcasted_iota(jnp.int32, (cols, LANES), 0)
    return row * LANES + lax.broadcasted_iota(jnp.int32, (cols, LANES), 1)


SPAN = LANES // 4
LEN, REWARD = 2 * SPAN, 3 * SPAN
STEPS = 8


def token_kernel(
    dests,
    small_hbm,
    policy_hbm,
    anchor_hbm,
    u_ref,
    sums_ref,
    slot_of,
    policy,
    anchor,
    parts,
    len_ref,
    reward_ref,
    prompt_ref,
    sem,
    small_sem,
):
    slots, width = policy.shape
    rows = slots // STEPS
    cols = width // LANES
    per_dest = slots // dests

    def loads(step):
        part = pl.ds(pl.multiple_of(step * rows, rows), rows)
        return (
            pltpu.make_async_copy(policy_hbm.at[part], policy.at[part], sem.at[0, step]),
            pltpu.make_async_copy(anchor_hbm.at[part], anchor.at[part], sem.at[1, step]),
        )

    small = [
        pltpu.make_async_copy(src, dst, small_sem.at[i])
        for i, (src, dst) in enumerate(zip(small_hbm, (prompt_ref, len_ref, reward_ref)))
    ]
    for load in (*loads(0), *small):
        load.start()
    for step in range(1, STEPS):
        for load in loads(step):
            load.start()
    for load in small:
        load.wait()

    def invert(s, carry):
        slot_of[0, prompt_ref[0, s] & (slots - 1)] = s
        return carry

    lax.fori_loop(0, slots, invert, 0, unroll=16)
    lane = lax.broadcasted_iota(jnp.int32, (8, LANES), 1)
    sub = lax.broadcasted_iota(jnp.int32, (8, LANES), 0)

    @pl.loop(0, STEPS)
    def _(step):
        for load in loads(step):
            load.wait()

        @pl.loop(0, rows // 8)
        def _(group):
            first = pl.multiple_of(step * rows + group * 8, 8)
            length = jnp.full((8, LANES), len_ref[0, first], jnp.int32)
            reward = jnp.full((8, LANES), reward_ref[0, first], jnp.int32)
            for i in range(1, 8):
                length = jnp.where(sub == i, len_ref[0, first + i], length)
                reward = jnp.where(sub == i, reward_ref[0, first + i], reward)
            sums_ref[pl.ds(first, 8), :] = jnp.where(lane < LEN + SPAN, length, reward).astype(
                jnp.float32
            )
            behind = lane - length
            sums_p = [jnp.zeros((8, LANES), jnp.float32)] * 4
            sums_q = [jnp.zeros((8, LANES), jnp.float32)] * 4
            for c in range(cols):
                at = (pl.ds(first, 8), pl.ds(c * LANES, LANES))
                a = policy[at]
                d = anchor[at] - a
                valid = behind < -c * LANES
                u = jnp.where(valid, jnp.exp(d) - 1.0, 0.0)
                u_ref[at] = u
                sums_q[c % 4] = sums_q[c % 4] + (u - jnp.where(valid, d, 0.0))
                sums_p[c % 4] = sums_p[c % 4] + jnp.where(valid, a, 0.0)
            parts[0, pl.ds(first, 8), :] = (sums_p[0] + sums_p[1]) + (sums_p[2] + sums_p[3])
            parts[1, pl.ds(first, 8), :] = (sums_q[0] + sums_q[1]) + (sums_q[2] + sums_q[3])

    lane = lax.broadcasted_iota(jnp.int32, (slots, LANES), 1)
    p, q = (
        x + pltpu.roll(x, SPAN, 1)
        for x in (x + pltpu.roll(x, 2 * SPAN, 1) for x in (parts[0], parts[1]))
    )
    rest = jnp.where(lane < 2 * SPAN, q, sums_ref[...])
    sums_ref[...] = jnp.where(lane < SPAN, p, rest)


def token_terms(lengths, rewards, prompts, policy, anchor, dests):
    slots, width = policy.shape
    vmem = pl.BlockSpec(memory_space=pltpu.VMEM)
    smem = pl.BlockSpec(memory_space=pltpu.SMEM)
    hbm = pl.BlockSpec(memory_space=pl.ANY)

    def body(*refs):
        token_kernel(dests, refs[:3], *refs[3:])

    return pl.pallas_call(
        body,
        out_shape=(
            jax.ShapeDtypeStruct((slots, width), jnp.float32),
            jax.ShapeDtypeStruct((slots, LANES), jnp.float32),
            jax.ShapeDtypeStruct((1, slots), jnp.int32),
        ),
        in_specs=[hbm] * 5,
        out_specs=(vmem, vmem, smem),
        scratch_shapes=[
            pltpu.VMEM((slots, width), jnp.float32),
            pltpu.VMEM((slots, width), jnp.float32),
            pltpu.VMEM((2, slots, LANES), jnp.float32),
            pltpu.SMEM((1, slots), jnp.int32),
            pltpu.SMEM((1, slots), jnp.int32),
            pltpu.SMEM((1, slots), jnp.int32),
            pltpu.SemaphoreType.DMA((2, STEPS)),
            pltpu.SemaphoreType.DMA((3,)),
        ],
        compiler_params=pltpu.CompilerParams(vmem_limit_bytes=24 << 20),
        cost_estimate=pl.CostEstimate(
            flops=40_000_000, bytes_accessed=12 * slots * width, transcendentals=slots * width
        ),
        name="token_terms",
    )(prompts, lengths, rewards, policy, anchor)


def pack_kernel(
    dests,
    per_dest,
    cols,
    slot_of,
    len_ref,
    tok_refs,
    u_ref,
    sums_ref,
    main,
    stage,
    in_order,
):
    slots = dests * per_dest
    chunk = META + FAST
    last = dests - 1

    def one_dest(dest, most, ref, base):
        def row(r, at):
            p = dest * per_dest + r
            s = slot_of[0, p]
            first = (s >> 3) * (8 * cols) + (s & 7)
            ref[pl.ds(at, cols), :] = u_ref[pl.ds(first, cols, stride=8), :]
            in_order[pl.ds(p, 1), :] = sums_ref[pl.ds(s, 1), :]
            return at + ((len_ref[0, s] + (LANES - 1)) >> 7)

        end = lax.fori_loop(0, per_dest, row, base + META, unroll=4)
        return jnp.maximum(most, end - base - META)

    def in_place(dest, most):
        return one_dest(dest, most, main, pl.multiple_of(dest * chunk, 8))

    most = lax.fori_loop(0, last, in_place, jnp.int32(0))
    most = one_dest(last, most, stage, 0)
    main[last * chunk + META : (last + 1) * chunk, :] = stage[META:chunk, :]

    sub = lax.broadcasted_iota(jnp.int32, (8, LANES), 0)
    lane = lax.broadcasted_iota(jnp.int32, (8, LANES), 1)
    pick = jnp.where((sub == 0) & (lane == LEN), 1.0, 0.0)
    pick = jnp.where((sub == 1) & (lane == REWARD), 0.25, pick)
    pick = jnp.where((sub == 2) & (lane < SPAN), 1.0, pick)
    pick = jnp.where((sub == 3) & (lane >= SPAN) & (lane < 2 * SPAN), 1.0, pick)
    head = lax.dot_general(
        pick,
        in_order[...],
        (((1,), (1,)), ((), ())),
        precision=lax.Precision.HIGHEST,
        preferred_element_type=jnp.float32,
    )
    tokens = jnp.sum(sum(t[...] for t in tok_refs).astype(jnp.float32), axis=1, keepdims=True)
    sub = lax.broadcasted_iota(jnp.int32, (8, slots), 0)
    head = jnp.where(sub == 4, tokens, head)
    head = jnp.where(sub == 5, most.astype(jnp.float32), head)
    for dest in range(dests):
        half = dest * per_dest // LANES * LANES
        main[dest * chunk : dest * chunk + META, :] = head[:, half : half + LANES]


def pack(slot_of, lengths, tokens, u, sums, dests):
    slots = lengths.shape[1]
    per_dest = slots // dests
    cols = u.shape[0] // slots
    chunk = META + FAST
    smem = pl.BlockSpec(memory_space=pltpu.SMEM)
    vmem = pl.BlockSpec(memory_space=pltpu.VMEM)

    def body(*refs):
        small, refs = refs[:2], refs[2:]
        tok_refs, refs = refs[: len(tokens)], refs[len(tokens) :]
        pack_kernel(dests, per_dest, cols, *small, tok_refs, *refs)

    return pl.pallas_call(
        body,
        out_shape=jax.ShapeDtypeStruct((dests * chunk, LANES), jnp.float32),
        in_specs=[smem] * 2 + [vmem] * (len(tokens) + 2),
        out_specs=vmem,
        scratch_shapes=[
            pltpu.VMEM((META + (per_dest + 1) * cols, LANES), jnp.float32),
            pltpu.VMEM((slots, LANES), jnp.float32),
        ],
        compiler_params=pltpu.CompilerParams(vmem_limit_bytes=24 << 20),
        name="pack",
    )(slot_of, lengths, *tokens, u, sums).reshape(dests, chunk, LANES)


def pack_rest(slot_of, lengths, u, dests):
    slots = lengths.shape[1]
    per_dest = slots // dests
    cols = u.shape[0] // slots
    spare = per_dest * cols - FAST

    def body(slot_of, len_ref, u_ref, rest_hbm, stage, sem):
        @pl.loop(0, dests)
        def _(dest):
            def row(r, at):
                s = slot_of[0, dest * per_dest + r]
                first = (s >> 3) * (8 * cols) + (s & 7)
                stage[pl.ds(at, cols), :] = u_ref[pl.ds(first, cols, stride=8), :]
                return at + ((len_ref[0, s] + (LANES - 1)) >> 7)

            lax.fori_loop(0, per_dest, row, jnp.int32(0))
            copy = pltpu.make_async_copy(stage.at[pl.ds(FAST, spare)], rest_hbm.at[dest], sem)
            copy.start()
            copy.wait()

    smem = pl.BlockSpec(memory_space=pltpu.SMEM)
    return pl.pallas_call(
        body,
        out_shape=jax.ShapeDtypeStruct((dests, spare, LANES), jnp.float32),
        in_specs=[smem, smem, pl.BlockSpec(memory_space=pltpu.VMEM)],
        out_specs=pl.BlockSpec(memory_space=pl.ANY),
        scratch_shapes=[
            pltpu.VMEM(((per_dest + 1) * cols, LANES), jnp.float32),
            pltpu.SemaphoreType.DMA,
        ],
        compiler_params=pltpu.CompilerParams(vmem_limit_bytes=16 << 20),
        name="pack_rest",
    )(slot_of, lengths, u)


def score_kernel(members, per_dest, cols, scales, refs):
    main, grad_hbm, loss_ref, adv_ref, table_ref, more_ref, tail, grad, numbers, num_sem, out_sem = refs
    grad_scale, loss_scale = scales
    width = per_dest * cols
    chunk = META + FAST

    def field(i):
        return jnp.concatenate(
            [main[k * chunk + i : k * chunk + i + 1, :] for k in range(members)], axis=0
        )

    start = lax.rem(lax.axis_index(GY) * per_dest, LANES)
    shift = lax.rem(LANES - start, LANES)
    lengths, reward, sums_p, sums_q = (pltpu.roll(field(i), shift, 1) for i in range(4))
    total = jnp.sum(reward, axis=0, keepdims=True)
    advantage = (members * reward - total) / (members - 1)
    tokens = jnp.sum(field(4), axis=0, keepdims=True)
    scale = grad_scale / tokens
    table_ref[0] = lengths
    table_ref[1] = -advantage * scale
    table_ref[2] = jnp.broadcast_to(scale * -KL, (members, LANES))
    to_scalars = pltpu.make_async_copy(table_ref, numbers, num_sem)
    to_scalars.start()
    loss = (KL * sums_q - advantage * sums_p) * (loss_scale / tokens)
    loss_ref[...] = loss[:, 0:per_dest]
    adv_ref[...] = advantage[:, 0:per_dest]
    most = jnp.max(field(5), axis=0, keepdims=True)
    more_ref[...] = jnp.where(most > FAST, 1, 0)
    position = sliced_position(cols)
    last = members - 1
    tail[0:chunk, :] = main[last * chunk : (last + 1) * chunk, :]
    to_scalars.wait()

    def out_copy(k):
        part = pl.ds(pl.multiple_of(k * width, width), width)
        return pltpu.make_async_copy(grad.at[part], grad_hbm.at[part], out_sem.at[k])

    def one_member(k, ref, base):
        slope = numbers[2, 0, 0]
        at = base + META
        for r in range(per_dest):
            length = numbers[0, k, r].astype(jnp.int32)
            u = ref[pl.ds(at, cols), :]
            y = jnp.where(position < length, numbers[1, k, r] + slope * u, 0.0)
            first = k * width + r // 8 * (8 * cols) + r % 8
            grad[pl.ds(first, cols, stride=8), :] = y
            at = jnp.minimum(at + ((length + (LANES - 1)) >> 7), base + chunk)
        out_copy(k).start()

    @pl.loop(0, last)
    def _(k):
        one_member(k, main, pl.multiple_of(k * chunk, 8))

    one_member(last, tail, 0)

    @pl.loop(0, members)
    def _(k):
        out_copy(k).wait()


def score(main, scales, per_dest, cols):
    members, chunk, _ = main.shape
    full = per_dest * cols
    hbm = pl.BlockSpec(memory_space=pl.ANY)
    vmem = pl.BlockSpec(memory_space=pltpu.VMEM)

    def body(*refs):
        score_kernel(members, per_dest, cols, scales, refs)

    small = jax.ShapeDtypeStruct((members, per_dest), jnp.float32)
    return pl.pallas_call(
        body,
        out_shape=(
            jax.ShapeDtypeStruct((members * full, LANES), jnp.float32),
            small,
            small,
            jax.ShapeDtypeStruct((3, members, LANES), jnp.float32),
            jax.ShapeDtypeStruct((1, LANES), jnp.int32),
        ),
        in_specs=[vmem],
        out_specs=(hbm, vmem, vmem, vmem, vmem),
        scratch_shapes=[
            pltpu.VMEM((chunk + cols, LANES), jnp.float32),
            pltpu.VMEM((members * full, LANES), jnp.float32),
            pltpu.SMEM((3, members, LANES), jnp.float32),
            pltpu.SemaphoreType.DMA,
            pltpu.SemaphoreType.DMA((members,)),
        ],
        compiler_params=pltpu.CompilerParams(vmem_limit_bytes=24 << 20),
        name="score",
    )(main.reshape(members * chunk, LANES))


def finish_kernel(members, per_dest, cols, refs):
    table_hbm, rest_hbm, _, grad_hbm, numbers, rest, grad, sem = refs
    width = per_dest * cols
    spare = width - FAST
    load = pltpu.make_async_copy(table_hbm, numbers, sem.at[0])
    load.start()
    load.wait()
    position = sliced_position(cols)
    row_of = lax.broadcasted_iota(jnp.int32, (cols, LANES), 0)

    @pl.loop(0, members)
    def _(k):
        place = grad_hbm.at[pl.ds(k * width, width)]
        loads = (
            pltpu.make_async_copy(rest_hbm.at[k], rest.at[pl.ds(cols, spare)], sem.at[0]),
            pltpu.make_async_copy(place, grad, sem.at[1]),
        )
        for load in loads:
            load.start()
        for load in loads:
            load.wait()

        def row(r, at):
            length = numbers[0, k, r].astype(jnp.int32)
            end = at + ((length + (LANES - 1)) >> 7)

            @pl.when(end > FAST)
            def _():
                u = rest[pl.ds(at - FAST + cols, cols), :]
                y = jnp.where(position < length, numbers[1, k, r] + numbers[2, 0, 0] * u, 0.0)
                first = (r >> 3) * (8 * cols) + (r & 7)
                old = grad[pl.ds(first, cols, stride=8), :]
                grad[pl.ds(first, cols, stride=8), :] = jnp.where(row_of + at >= FAST, y, old)

            return end

        lax.fori_loop(0, per_dest, row, jnp.int32(0))
        store = pltpu.make_async_copy(grad, place, sem.at[1])
        store.start()
        store.wait()


def finish(grad, rest, table, per_dest, cols):
    members = rest.shape[0]
    full = per_dest * cols
    hbm = pl.BlockSpec(memory_space=pl.ANY)

    def body(*refs):
        finish_kernel(members, per_dest, cols, refs)

    return pl.pallas_call(
        body,
        out_shape=jax.ShapeDtypeStruct(grad.shape, jnp.float32),
        in_specs=[hbm, hbm, hbm],
        out_specs=hbm,
        input_output_aliases={2: 0},
        scratch_shapes=[
            pltpu.SMEM((3, members, LANES), jnp.float32),
            pltpu.VMEM((full - FAST + 2 * cols, LANES), jnp.float32),
            pltpu.VMEM((full, LANES), jnp.float32),
            pltpu.SemaphoreType.DMA((2,)),
        ],
        compiler_params=pltpu.CompilerParams(vmem_limit_bytes=8 << 20),
        name="finish",
    )(table, rest, grad)


def peers(x, axis):
    size = lax.axis_size(axis)
    return [
        lax.ppermute(x, axis, [(i, i ^ step) for i in range(size)])
        for step in range(1, size)
    ]


def body(policy_logp, anchor_logp, lengths, rewards, slot_prompt):
    members_dev, slots, seq_slots = policy_logp.shape
    dests = lax.axis_size(GY)
    per_dest = slots // dests
    cols = seq_slots // LANES
    members = members_dev * dests
    samples = members * slots * lax.axis_size(GX)
    scales = (float(samples * seq_slots), float(samples))
    tokens = [lengths] + peers(lengths, GX)
    u, sums, slot_of = token_terms(
        *(
            pltpu.with_memory_space_constraint(x, pltpu.HBM)
            for x in (lengths, rewards, slot_prompt, policy_logp[0], anchor_logp[0])
        ),
        dests,
    )
    u = lane_rows(u, slots, seq_slots)
    main = pack(slot_of, lengths, tokens, u, sums, dests)
    main = lax.all_to_all(main, GY, 0, 0, tiled=True)
    grad, loss, advantage, table, more = score(main, scales, per_dest, cols)

    def the_rest(state):
        grad, _ = state
        rest = pack_rest(slot_of, lengths, u, dests)
        got = lax.all_to_all(rest, GY, 0, 0, tiled=True)
        return finish(grad, got, table, per_dest, cols), jnp.int32(0)

    grad, _ = lax.while_loop(lambda state: state[1] > 0, the_rest, (grad, more[0, 0]))
    grad = (
        grad.reshape(members, per_dest // 8, cols, 8, LANES)
        .transpose(0, 1, 3, 2, 4)
        .reshape(members, per_dest, seq_slots)
    )
    return grad, loss, advantage


def solution(mesh):
    torus = Mesh(mesh.devices.reshape(4, 2, 4, 4), ("gx_0", "gx_1", "gy_0", "gy_1"))
    return jax.shard_map(
        body,
        mesh=torus,
        in_specs=(P(GY, GX, None), P(GY, GX, None), P(GY, GX), P(GY, GX), P(GY, GX)),
        out_specs=(P(None, GX_GY, None), P(None, GX_GY), P(None, GX_GY)),
        check_vma=False,
    )
```

```python
import jax
import jax.numpy as jnp
from jax import lax
from jax.experimental import pallas as pl
from jax.experimental.pallas import tpu as pltpu
from jax.sharding import Mesh
from jax.sharding import PartitionSpec as P

GX_GY = ("gx_0", "gx_1", "gy_0", "gy_1")
GY = ("gy_0", "gy_1")
GX = ("gx_0", "gx_1")

KL = 0.1
LANES = 128
META = 8
FAST = 432


def sliced_position(cols):
    row = lax.broadcasted_iota(jnp.int32, (cols, LANES), 0)
    return row * LANES + lax.broadcasted_iota(jnp.int32, (cols, LANES), 1)


SPAN = LANES // 4
LEN, REWARD = 2 * SPAN, 3 * SPAN
STEPS = 8


def token_kernel(
    dests,
    small_hbm,
    policy_hbm,
    anchor_hbm,
    u_ref,
    sums_ref,
    slot_of,
    policy,
    anchor,
    parts,
    len_ref,
    reward_ref,
    prompt_ref,
    sem,
    small_sem,
):
    slots, width = policy.shape
    rows = slots // STEPS
    cols = width // LANES
    per_dest = slots // dests

    def loads(step):
        part = pl.ds(pl.multiple_of(step * rows, rows), rows)
        return (
            pltpu.make_async_copy(policy_hbm.at[part], policy.at[part], sem.at[0, step]),
            pltpu.make_async_copy(anchor_hbm.at[part], anchor.at[part], sem.at[1, step]),
        )

    small = [
        pltpu.make_async_copy(src, dst, small_sem.at[i])
        for i, (src, dst) in enumerate(zip(small_hbm, (prompt_ref, len_ref, reward_ref)))
    ]
    for load in small:
        load.start()
    for step in range(STEPS):
        for load in loads(step):
            load.start()
    for load in small:
        load.wait()

    def invert(s, carry):
        slot_of[0, prompt_ref[0, s] & (slots - 1)] = s
        return carry

    lax.fori_loop(0, slots, invert, 0, unroll=16)
    lane = lax.broadcasted_iota(jnp.int32, (8, LANES), 1)
    sub = lax.broadcasted_iota(jnp.int32, (8, LANES), 0)

    @pl.loop(0, STEPS)
    def _(step):
        for load in loads(step):
            load.wait()

        @pl.loop(0, rows // 8)
        def _(group):
            first = pl.multiple_of(step * rows + group * 8, 8)
            length = jnp.full((8, LANES), len_ref[0, first], jnp.int32)
            reward = jnp.full((8, LANES), reward_ref[0, first], jnp.int32)
            for i in range(1, 8):
                length = jnp.where(sub == i, len_ref[0, first + i], length)
                reward = jnp.where(sub == i, reward_ref[0, first + i], reward)
            sums_ref[pl.ds(first, 8), :] = jnp.where(lane < LEN + SPAN, length, reward).astype(
                jnp.float32
            )
            behind = lane - length
            sums_p = [jnp.zeros((8, LANES), jnp.float32)] * 4
            sums_q = [jnp.zeros((8, LANES), jnp.float32)] * 4
            for c in range(cols):
                at = (pl.ds(first, 8), pl.ds(c * LANES, LANES))
                a = policy[at]
                d = anchor[at] - a
                valid = behind < -c * LANES
                u = jnp.where(valid, jnp.exp(d) - 1.0, 0.0)
                u_ref[pl.ds(first * cols + c // 8 * 64 + c % 8, 8, stride=8), :] = u
                sums_q[c % 4] = sums_q[c % 4] + (u - jnp.where(valid, d, 0.0))
                sums_p[c % 4] = sums_p[c % 4] + jnp.where(valid, a, 0.0)
            parts[0, pl.ds(first, 8), :] = (sums_p[0] + sums_p[1]) + (sums_p[2] + sums_p[3])
            parts[1, pl.ds(first, 8), :] = (sums_q[0] + sums_q[1]) + (sums_q[2] + sums_q[3])

    lane = lax.broadcasted_iota(jnp.int32, (slots, LANES), 1)
    p, q = (
        x + pltpu.roll(x, SPAN, 1)
        for x in (x + pltpu.roll(x, 2 * SPAN, 1) for x in (parts[0], parts[1]))
    )
    rest = jnp.where(lane < 2 * SPAN, q, sums_ref[...])
    sums_ref[...] = jnp.where(lane < SPAN, p, rest)


def token_terms(lengths, rewards, prompts, policy, anchor, dests):
    slots, width = policy.shape
    vmem = pl.BlockSpec(memory_space=pltpu.VMEM)
    smem = pl.BlockSpec(memory_space=pltpu.SMEM)
    hbm = pl.BlockSpec(memory_space=pl.ANY)

    def body(*refs):
        token_kernel(dests, refs[:3], *refs[3:])

    return pl.pallas_call(
        body,
        out_shape=(
            jax.ShapeDtypeStruct((slots * width // LANES, LANES), jnp.float32),
            jax.ShapeDtypeStruct((slots, LANES), jnp.float32),
            jax.ShapeDtypeStruct((1, slots), jnp.int32),
        ),
        in_specs=[hbm] * 5,
        out_specs=(vmem, vmem, smem),
        scratch_shapes=[
            pltpu.VMEM((slots, width), jnp.float32),
            pltpu.VMEM((slots, width), jnp.float32),
            pltpu.VMEM((2, slots, LANES), jnp.float32),
            pltpu.SMEM((1, slots), jnp.int32),
            pltpu.SMEM((1, slots), jnp.int32),
            pltpu.SMEM((1, slots), jnp.int32),
            pltpu.SemaphoreType.DMA((2, STEPS)),
            pltpu.SemaphoreType.DMA((3,)),
        ],
        compiler_params=pltpu.CompilerParams(vmem_limit_bytes=24 << 20),
        cost_estimate=pl.CostEstimate(
            flops=40_000_000, bytes_accessed=12 * slots * width, transcendentals=slots * width
        ),
        name="token_terms",
    )(prompts, lengths, rewards, policy, anchor)


def pack_kernel(
    dests,
    per_dest,
    cols,
    slot_of,
    len_ref,
    u_ref,
    sums_ref,
    main,
    head_ref,
    stage,
    in_order,
):
    slots = dests * per_dest
    chunk = META + FAST
    last = dests - 1

    def one_dest(dest, most, ref, base):
        def row(r, at):
            p = dest * per_dest + r
            s = slot_of[0, p]
            first = pl.multiple_of((s >> 3) * (8 * cols) + (s & 7) * 8, 8)
            for j in range(cols // 8):
                ref[pl.ds(at + 8 * j, 8), :] = u_ref[pl.ds(first + 64 * j, 8), :]
            in_order[pl.ds(p, 1), :] = sums_ref[pl.ds(s, 1), :]
            return at + ((len_ref[0, s] + (LANES - 1)) >> 7)

        end = lax.fori_loop(0, per_dest, row, base + META, unroll=4)
        return jnp.maximum(most, end - base - META)

    def in_place(dest, most):
        return one_dest(dest, most, main, pl.multiple_of(dest * chunk, 8))

    most = lax.fori_loop(0, last, in_place, jnp.int32(0))
    most = one_dest(last, most, stage, 0)
    main[last * chunk + META : (last + 1) * chunk, :] = stage[META:chunk, :]

    sub = lax.broadcasted_iota(jnp.int32, (8, LANES), 0)
    lane = lax.broadcasted_iota(jnp.int32, (8, LANES), 1)
    pick = jnp.where((sub == 0) & (lane == LEN), 1.0, 0.0)
    pick = jnp.where((sub == 1) & (lane == REWARD), 0.25, pick)
    pick = jnp.where((sub == 2) & (lane < SPAN), 1.0, pick)
    pick = jnp.where((sub == 3) & (lane >= SPAN) & (lane < 2 * SPAN), 1.0, pick)
    head = lax.dot_general(
        pick,
        in_order[...],
        (((1,), (1,)), ((), ())),
        precision=lax.Precision.HIGHEST,
        preferred_element_type=jnp.float32,
    )
    sub = lax.broadcasted_iota(jnp.int32, (8, slots), 0)
    head_ref[...] = jnp.where(sub == 5, most.astype(jnp.float32), head)


def stamp_kernel(dests, per_dest, head, counts, _, main, tile, sem):
    sub = lax.broadcasted_iota(jnp.int32, (8, LANES), 0)
    count = jnp.sum(sum(c[...] for c in counts).astype(jnp.float32), axis=1, keepdims=True)
    halves = head.shape[1] // LANES
    for half in range(halves):
        tile[half] = jnp.where(sub == 4, count, head[:, half * LANES : (half + 1) * LANES])
    copies = [
        pltpu.make_async_copy(
            tile.at[dest * per_dest // LANES], main.at[dest, pl.ds(0, META)], sem.at[dest]
        )
        for dest in range(dests)
    ]
    for copy in copies:
        copy.start()
    for copy in copies:
        copy.wait()


def stamp(head, counts, main, per_dest):
    dests = main.shape[0]
    vmem = pl.BlockSpec(memory_space=pltpu.VMEM)
    place = pl.BlockSpec(memory_space=pl.ANY)

    def body(head, *refs):
        stamp_kernel(dests, per_dest, head, refs[: len(counts)], *refs[len(counts) :])

    return pl.pallas_call(
        body,
        out_shape=jax.ShapeDtypeStruct(main.shape, jnp.float32),
        in_specs=[vmem] * (1 + len(counts)) + [place],
        out_specs=place,
        input_output_aliases={1 + len(counts): 0},
        scratch_shapes=[
            pltpu.VMEM((head.shape[1] // LANES, META, LANES), jnp.float32),
            pltpu.SemaphoreType.DMA((dests,)),
        ],
        compiler_params=pltpu.CompilerParams(vmem_limit_bytes=4 << 20),
        name="stamp",
    )(head, *counts, main)


def added(x, y, after):
    def body(x, y, _, out):
        out[...] = x[...] + y[...]

    vmem = pl.BlockSpec(memory_space=pltpu.VMEM)
    return pl.pallas_call(
        body,
        out_shape=jax.ShapeDtypeStruct(x.shape, x.dtype),
        in_specs=[vmem, vmem, pl.BlockSpec(memory_space=pl.ANY)],
        out_specs=vmem,
        compiler_params=pltpu.CompilerParams(vmem_limit_bytes=4 << 20),
        name="added",
    )(x, y, after)


def pack(slot_of, lengths, u, sums, dests):
    slots = lengths.shape[1]
    per_dest = slots // dests
    cols = u.shape[0] // slots
    chunk = META + FAST
    smem = pl.BlockSpec(memory_space=pltpu.SMEM)
    vmem = pl.BlockSpec(memory_space=pltpu.VMEM)

    def body(*refs):
        pack_kernel(dests, per_dest, cols, *refs)

    main, head = pl.pallas_call(
        body,
        out_shape=(
            jax.ShapeDtypeStruct((dests * chunk, LANES), jnp.float32),
            jax.ShapeDtypeStruct((META, slots), jnp.float32),
        ),
        in_specs=[smem] * 2 + [vmem] * 2,
        out_specs=(vmem, vmem),
        scratch_shapes=[
            pltpu.VMEM((META + (per_dest + 1) * cols, LANES), jnp.float32),
            pltpu.VMEM((slots, LANES), jnp.float32),
        ],
        compiler_params=pltpu.CompilerParams(vmem_limit_bytes=24 << 20),
        cost_estimate=pl.CostEstimate(
            flops=40_000_000, bytes_accessed=8 * dests * chunk * LANES, transcendentals=0
        ),
        name="pack",
    )(slot_of, lengths, u, sums)
    return main.reshape(dests, chunk, LANES), head


def pack_rest(slot_of, lengths, u, dests):
    slots = lengths.shape[1]
    per_dest = slots // dests
    cols = u.shape[0] // slots
    spare = per_dest * cols - FAST

    def body(slot_of, len_ref, u_ref, rest_hbm, stage, sem):
        @pl.loop(0, dests)
        def _(dest):
            def row(r, at):
                s = slot_of[0, dest * per_dest + r]
                first = pl.multiple_of((s >> 3) * (8 * cols) + (s & 7) * 8, 8)
                for j in range(cols // 8):
                    stage[pl.ds(at + 8 * j, 8), :] = u_ref[pl.ds(first + 64 * j, 8), :]
                return at + ((len_ref[0, s] + (LANES - 1)) >> 7)

            lax.fori_loop(0, per_dest, row, jnp.int32(0))
            copy = pltpu.make_async_copy(stage.at[pl.ds(FAST, spare)], rest_hbm.at[dest], sem)
            copy.start()
            copy.wait()

    smem = pl.BlockSpec(memory_space=pltpu.SMEM)
    return pl.pallas_call(
        body,
        out_shape=jax.ShapeDtypeStruct((dests, spare, LANES), jnp.float32),
        in_specs=[smem, smem, pl.BlockSpec(memory_space=pltpu.VMEM)],
        out_specs=pl.BlockSpec(memory_space=pl.ANY),
        scratch_shapes=[
            pltpu.VMEM(((per_dest + 1) * cols, LANES), jnp.float32),
            pltpu.SemaphoreType.DMA,
        ],
        compiler_params=pltpu.CompilerParams(vmem_limit_bytes=16 << 20),
        name="pack_rest",
    )(slot_of, lengths, u)


def score_kernel(members, per_dest, cols, scales, refs):
    main, grad_hbm, loss_ref, adv_ref, table_ref, more_ref, tail, grad, numbers, num_sem, out_sem = refs
    grad_scale, loss_scale = scales
    width = per_dest * cols
    chunk = META + FAST

    def field(i):
        return jnp.concatenate(
            [main[k * chunk + i : k * chunk + i + 1, :] for k in range(members)], axis=0
        )

    start = lax.rem(lax.axis_index(GY) * per_dest, LANES)
    shift = lax.rem(LANES - start, LANES)
    lengths, reward, sums_p, sums_q = (pltpu.roll(field(i), shift, 1) for i in range(4))
    total = jnp.sum(reward, axis=0, keepdims=True)
    advantage = (members * reward - total) / (members - 1)
    tokens = jnp.sum(field(4), axis=0, keepdims=True)
    scale = grad_scale / tokens
    table_ref[0] = lengths
    table_ref[1] = -advantage * scale
    table_ref[2] = jnp.broadcast_to(scale * -KL, (members, LANES))
    to_scalars = pltpu.make_async_copy(table_ref, numbers, num_sem)
    to_scalars.start()
    loss = (KL * sums_q - advantage * sums_p) * (loss_scale / tokens)
    loss_ref[...] = loss[:, 0:per_dest]
    adv_ref[...] = advantage[:, 0:per_dest]
    most = jnp.max(field(5), axis=0, keepdims=True)
    more_ref[...] = jnp.where(most > FAST, 1, 0)
    position = sliced_position(cols)
    last = members - 1
    tail[0:chunk, :] = main[last * chunk : (last + 1) * chunk, :]
    to_scalars.wait()

    def out_copy(k):
        part = pl.ds(pl.multiple_of(k * width, width), width)
        return pltpu.make_async_copy(grad.at[part], grad_hbm.at[part], out_sem.at[k])

    def one_member(k, ref, base):
        slope = numbers[2, 0, 0]
        at = base + META
        for r in range(per_dest):
            length = numbers[0, k, r].astype(jnp.int32)
            u = ref[pl.ds(at, cols), :]
            y = jnp.where(position < length, numbers[1, k, r] + slope * u, 0.0)
            first = k * width + r // 8 * (8 * cols) + r % 8
            grad[pl.ds(first, cols, stride=8), :] = y
            at = jnp.minimum(at + ((length + (LANES - 1)) >> 7), base + chunk)
        out_copy(k).start()

    @pl.loop(0, last)
    def _(k):
        one_member(k, main, pl.multiple_of(k * chunk, 8))

    one_member(last, tail, 0)

    @pl.loop(0, members)
    def _(k):
        out_copy(k).wait()


def score(main, scales, per_dest, cols):
    members, chunk, _ = main.shape
    full = per_dest * cols
    hbm = pl.BlockSpec(memory_space=pl.ANY)
    vmem = pl.BlockSpec(memory_space=pltpu.VMEM)

    def body(*refs):
        score_kernel(members, per_dest, cols, scales, refs)

    small = jax.ShapeDtypeStruct((members, per_dest), jnp.float32)
    return pl.pallas_call(
        body,
        out_shape=(
            jax.ShapeDtypeStruct((members * full, LANES), jnp.float32),
            small,
            small,
            jax.ShapeDtypeStruct((3, members, LANES), jnp.float32),
            jax.ShapeDtypeStruct((1, LANES), jnp.int32),
        ),
        in_specs=[vmem],
        out_specs=(hbm, vmem, vmem, vmem, vmem),
        scratch_shapes=[
            pltpu.VMEM((chunk + cols, LANES), jnp.float32),
            pltpu.VMEM((members * full, LANES), jnp.float32),
            pltpu.SMEM((3, members, LANES), jnp.float32),
            pltpu.SemaphoreType.DMA,
            pltpu.SemaphoreType.DMA((members,)),
        ],
        compiler_params=pltpu.CompilerParams(vmem_limit_bytes=24 << 20),
        name="score",
    )(main.reshape(members * chunk, LANES))


def finish_kernel(members, per_dest, cols, refs):
    table_hbm, rest_hbm, _, grad_hbm, numbers, rest, grad, sem = refs
    width = per_dest * cols
    spare = width - FAST
    load = pltpu.make_async_copy(table_hbm, numbers, sem.at[0])
    load.start()
    load.wait()
    position = sliced_position(cols)
    row_of = lax.broadcasted_iota(jnp.int32, (cols, LANES), 0)

    @pl.loop(0, members)
    def _(k):
        place = grad_hbm.at[pl.ds(k * width, width)]
        loads = (
            pltpu.make_async_copy(rest_hbm.at[k], rest.at[pl.ds(cols, spare)], sem.at[0]),
            pltpu.make_async_copy(place, grad, sem.at[1]),
        )
        for load in loads:
            load.start()
        for load in loads:
            load.wait()

        def row(r, at):
            length = numbers[0, k, r].astype(jnp.int32)
            end = at + ((length + (LANES - 1)) >> 7)

            @pl.when(end > FAST)
            def _():
                u = rest[pl.ds(at - FAST + cols, cols), :]
                y = jnp.where(position < length, numbers[1, k, r] + numbers[2, 0, 0] * u, 0.0)
                first = (r >> 3) * (8 * cols) + (r & 7)
                old = grad[pl.ds(first, cols, stride=8), :]
                grad[pl.ds(first, cols, stride=8), :] = jnp.where(row_of + at >= FAST, y, old)

            return end

        lax.fori_loop(0, per_dest, row, jnp.int32(0))
        store = pltpu.make_async_copy(grad, place, sem.at[1])
        store.start()
        store.wait()


def finish(grad, rest, table, per_dest, cols):
    members = rest.shape[0]
    full = per_dest * cols
    hbm = pl.BlockSpec(memory_space=pl.ANY)

    def body(*refs):
        finish_kernel(members, per_dest, cols, refs)

    return pl.pallas_call(
        body,
        out_shape=jax.ShapeDtypeStruct(grad.shape, jnp.float32),
        in_specs=[hbm, hbm, hbm],
        out_specs=hbm,
        input_output_aliases={2: 0},
        scratch_shapes=[
            pltpu.SMEM((3, members, LANES), jnp.float32),
            pltpu.VMEM((full - FAST + 2 * cols, LANES), jnp.float32),
            pltpu.VMEM((full, LANES), jnp.float32),
            pltpu.SemaphoreType.DMA((2,)),
        ],
        compiler_params=pltpu.CompilerParams(vmem_limit_bytes=8 << 20),
        name="finish",
    )(table, rest, grad)


def peers(x, axis):
    size = lax.axis_size(axis)
    return [
        lax.ppermute(x, axis, [(i, i ^ step) for i in range(size)])
        for step in range(1, size)
    ]


def body(policy_logp, anchor_logp, lengths, rewards, slot_prompt):
    members_dev, slots, seq_slots = policy_logp.shape
    dests = lax.axis_size(GY)
    per_dest = slots // dests
    cols = seq_slots // LANES
    members = members_dev * dests
    samples = members * slots * lax.axis_size(GX)
    scales = (float(samples * seq_slots), float(samples))
    other = peers(lengths, "gx_1")[0]
    u, sums, slot_of = token_terms(
        *(
            pltpu.with_memory_space_constraint(x, pltpu.HBM)
            for x in (lengths, rewards, slot_prompt, policy_logp[0], anchor_logp[0])
        ),
        dests,
    )
    pair = added(lengths, other, slot_of)
    main, head = pack(slot_of, lengths, u, sums, dests)
    main = stamp(head, [pair] + peers(pair, "gx_0"), main, per_dest)
    main = lax.all_to_all(main, GY, 0, 0, tiled=True)
    grad, loss, advantage, table, more = score(main, scales, per_dest, cols)

    def the_rest(state):
        grad, _ = state
        rest = pack_rest(slot_of, lengths, u, dests)
        got = lax.all_to_all(rest, GY, 0, 0, tiled=True)
        return finish(grad, got, table, per_dest, cols), jnp.int32(0)

    grad, _ = lax.while_loop(lambda state: state[1] > 0, the_rest, (grad, more[0, 0]))
    grad = (
        grad.reshape(members, per_dest // 8, cols, 8, LANES)
        .transpose(0, 1, 3, 2, 4)
        .reshape(members, per_dest, seq_slots)
    )
    return grad, loss, advantage


def solution(mesh):
    torus = Mesh(mesh.devices.reshape(4, 2, 4, 4), ("gx_0", "gx_1", "gy_0", "gy_1"))
    return jax.shard_map(
        body,
        mesh=torus,
        in_specs=(P(GY, GX, None), P(GY, GX, None), P(GY, GX), P(GY, GX), P(GY, GX)),
        out_specs=(P(None, GX_GY, None), P(None, GX_GY), P(None, GX_GY)),
        check_vma=False,
    )
```

```python
import jax
import jax.numpy as jnp
from jax import lax
from jax.experimental import pallas as pl
from jax.experimental.pallas import tpu as pltpu
from jax.sharding import Mesh
from jax.sharding import PartitionSpec as P

GX_GY = ("gx_0", "gx_1", "gy_0", "gy_1")
GY = ("gy_0", "gy_1")
GX = ("gx_0", "gx_1")

KL = 0.1
LANES = 128
META = 8
FAST = 432


def sliced_position(cols):
    row = lax.broadcasted_iota(jnp.int32, (cols, LANES), 0)
    return row * LANES + lax.broadcasted_iota(jnp.int32, (cols, LANES), 1)


SPAN = LANES // 4
LEN, SUM_P, REWARD, SUM_Q = (i * SPAN for i in range(4))
STEPS = 8


def token_kernel(
    dests,
    small_hbm,
    policy_hbm,
    anchor_hbm,
    u_ref,
    sums_ref,
    slot_hbm,
    policy,
    anchor,
    parts,
    len_ref,
    reward_ref,
    prompt_ref,
    slot_of,
    sem,
    small_sem,
):
    slots, width = policy.shape
    rows = slots // STEPS
    cols = width // LANES
    per_dest = slots // dests

    def loads(step):
        part = pl.ds(pl.multiple_of(step * rows, rows), rows)
        return (
            pltpu.make_async_copy(policy_hbm.at[part], policy.at[part], sem.at[0, step]),
            pltpu.make_async_copy(anchor_hbm.at[part], anchor.at[part], sem.at[1, step]),
        )

    small = [
        pltpu.make_async_copy(src, dst, small_sem.at[i])
        for i, (src, dst) in enumerate(zip(small_hbm, (prompt_ref, len_ref, reward_ref)))
    ]
    for load in small:
        load.start()
    for step in range(STEPS):
        for load in loads(step):
            load.start()
    for load in small:
        load.wait()

    def invert(s, carry):
        slot_of[0, prompt_ref[0, s] & (slots - 1)] = s
        return carry

    lax.fori_loop(0, slots, invert, 0, unroll=16)
    inverse = pltpu.make_async_copy(slot_of, slot_hbm, small_sem.at[3])
    inverse.start()
    lane = lax.broadcasted_iota(jnp.int32, (8, LANES), 1)
    sub = lax.broadcasted_iota(jnp.int32, (8, LANES), 0)

    @pl.loop(0, STEPS)
    def _(step):
        for load in loads(step):
            load.wait()

        @pl.loop(0, rows // 8)
        def _(group):
            first = pl.multiple_of(step * rows + group * 8, 8)
            length = jnp.full((8, LANES), len_ref[0, first], jnp.int32)
            reward = jnp.full((8, LANES), reward_ref[0, first], jnp.int32)
            for i in range(1, 8):
                length = jnp.where(sub == i, len_ref[0, first + i], length)
                reward = jnp.where(sub == i, reward_ref[0, first + i], reward)
            sums_ref[pl.ds(first, 8), :] = jnp.where(lane < REWARD, length, reward).astype(
                jnp.float32
            )
            behind = lane - length
            sums_p = [jnp.zeros((8, LANES), jnp.float32)] * 4
            sums_q = [jnp.zeros((8, LANES), jnp.float32)] * 4
            for c in range(cols):
                at = (pl.ds(first, 8), pl.ds(c * LANES, LANES))
                a = policy[at]
                d = anchor[at] - a
                valid = behind < -c * LANES
                u = jnp.exp(d) - 1.0
                u_ref[pl.ds(first * cols + c // 8 * 64 + c % 8, 8, stride=8), :] = u
                sums_q[c % 4] = sums_q[c % 4] + jnp.where(valid, u - d, 0.0)
                sums_p[c % 4] = sums_p[c % 4] + jnp.where(valid, a, 0.0)
            parts[0, pl.ds(first, 8), :] = (sums_p[0] + sums_p[1]) + (sums_p[2] + sums_p[3])
            parts[1, pl.ds(first, 8), :] = (sums_q[0] + sums_q[1]) + (sums_q[2] + sums_q[3])

    inverse.wait()
    lane = lax.broadcasted_iota(jnp.int32, (slots, LANES), 1)
    p, q = (x + pltpu.roll(x, 2 * SPAN, 1) for x in (parts[0], parts[1]))
    both = jnp.where(lane < REWARD, p, q)
    both = both + pltpu.roll(both, SPAN, 1)
    summed = (lane >= SUM_P) & (lane < REWARD) | (lane >= SUM_Q)
    sums_ref[...] = jnp.where(summed, both, sums_ref[...])


def token_terms(lengths, rewards, prompts, policy, anchor, dests):
    slots, width = policy.shape
    vmem = pl.BlockSpec(memory_space=pltpu.VMEM)
    hbm = pl.BlockSpec(memory_space=pl.ANY)

    def body(*refs):
        token_kernel(dests, refs[:3], *refs[3:])

    return pl.pallas_call(
        body,
        out_shape=(
            jax.ShapeDtypeStruct((slots * width // LANES, LANES), jnp.float32),
            jax.ShapeDtypeStruct((slots, LANES), jnp.float32),
            jax.ShapeDtypeStruct((1, slots), jnp.int32),
        ),
        in_specs=[hbm] * 5,
        out_specs=(vmem, vmem, hbm),
        scratch_shapes=[
            pltpu.VMEM((slots, width), jnp.float32),
            pltpu.VMEM((slots, width), jnp.float32),
            pltpu.VMEM((2, slots, LANES), jnp.float32),
            pltpu.SMEM((1, slots), jnp.int32),
            pltpu.SMEM((1, slots), jnp.int32),
            pltpu.SMEM((1, slots), jnp.int32),
            pltpu.SMEM((1, slots), jnp.int32),
            pltpu.SemaphoreType.DMA((2, STEPS)),
            pltpu.SemaphoreType.DMA((4,)),
        ],
        compiler_params=pltpu.CompilerParams(vmem_limit_bytes=24 << 20),
        cost_estimate=pl.CostEstimate(
            flops=40_000_000, bytes_accessed=12 * slots * width, transcendentals=slots * width
        ),
        name="token_terms",
    )(prompts, lengths, rewards, policy, anchor)


def pack_kernel(
    dests,
    per_dest,
    cols,
    slot_of,
    len_ref,
    u_ref,
    sums_ref,
    main,
    head_ref,
    stage,
    in_order,
):
    slots = dests * per_dest
    chunk = META + FAST
    last = dests - 1

    def one_dest(dest, most, ref, base):
        def row(r, at):
            p = dest * per_dest + r
            s = slot_of[0, p]
            first = pl.multiple_of((s >> 3) * (8 * cols) + (s & 7) * 8, 8)
            for j in range(cols // 8):
                ref[pl.ds(at + 8 * j, 8), :] = u_ref[pl.ds(first + 64 * j, 8), :]
            in_order[pl.ds(p, 1), :] = sums_ref[pl.ds(s, 1), :]
            return at + ((len_ref[0, s] + (LANES - 1)) >> 7)

        end = lax.fori_loop(0, per_dest, row, base + META, unroll=4)
        return jnp.maximum(most, end - base - META)

    def in_place(dest, most):
        return one_dest(dest, most, main, pl.multiple_of(dest * chunk, 8))

    most = lax.fori_loop(0, last, in_place, jnp.int32(0))
    most = one_dest(last, most, stage, 0)
    main[last * chunk + META : (last + 1) * chunk, :] = stage[META:chunk, :]

    sub = lax.broadcasted_iota(jnp.int32, (8, LANES), 0)
    lane = lax.broadcasted_iota(jnp.int32, (8, LANES), 1)
    pick = jnp.where((sub == 0) & (lane == LEN), 1.0, 0.0)
    pick = jnp.where((sub == 1) & (lane == REWARD), 0.25, pick)
    pick = jnp.where((sub == 2) & (lane >= SUM_P) & (lane < REWARD), 1.0, pick)
    pick = jnp.where((sub == 3) & (lane >= SUM_Q), 1.0, pick)
    head = lax.dot_general(
        pick,
        in_order[...],
        (((1,), (1,)), ((), ())),
        precision=lax.Precision.HIGHEST,
        preferred_element_type=jnp.float32,
    )
    sub = lax.broadcasted_iota(jnp.int32, (8, slots), 0)
    head_ref[...] = jnp.where(sub == 5, most.astype(jnp.float32), head)


def stamp_kernel(dests, per_dest, head, counts, _, main, tile, sem):
    sub = lax.broadcasted_iota(jnp.int32, (8, LANES), 0)
    count = jnp.sum(sum(c[...] for c in counts).astype(jnp.float32), axis=1, keepdims=True)
    halves = head.shape[1] // LANES
    for half in range(halves):
        tile[half] = jnp.where(sub == 4, count, head[:, half * LANES : (half + 1) * LANES])
    copies = [
        pltpu.make_async_copy(
            tile.at[dest * per_dest // LANES], main.at[dest, pl.ds(0, META)], sem.at[dest]
        )
        for dest in range(dests)
    ]
    for copy in copies:
        copy.start()
    for copy in copies:
        copy.wait()


def stamp(head, counts, main, per_dest):
    dests = main.shape[0]
    vmem = pl.BlockSpec(memory_space=pltpu.VMEM)
    place = pl.BlockSpec(memory_space=pl.ANY)

    def body(head, *refs):
        stamp_kernel(dests, per_dest, head, refs[: len(counts)], *refs[len(counts) :])

    return pl.pallas_call(
        body,
        out_shape=jax.ShapeDtypeStruct(main.shape, jnp.float32),
        in_specs=[vmem] * (1 + len(counts)) + [place],
        out_specs=place,
        input_output_aliases={1 + len(counts): 0},
        scratch_shapes=[
            pltpu.VMEM((head.shape[1] // LANES, META, LANES), jnp.float32),
            pltpu.SemaphoreType.DMA((dests,)),
        ],
        compiler_params=pltpu.CompilerParams(vmem_limit_bytes=4 << 20),
        name="stamp",
    )(head, *counts, main)


def added(parts, after):
    def body(*refs):
        refs[-1][...] = sum(x[...] for x in refs[:-2])

    vmem = pl.BlockSpec(memory_space=pltpu.VMEM)
    return pl.pallas_call(
        body,
        out_shape=jax.ShapeDtypeStruct(parts[0].shape, parts[0].dtype),
        in_specs=[vmem] * len(parts) + [pl.BlockSpec(memory_space=pl.ANY)],
        out_specs=vmem,
        compiler_params=pltpu.CompilerParams(vmem_limit_bytes=4 << 20),
        name="added",
    )(*parts, after)


def pack(slot_of, lengths, u, sums, dests):
    slots = lengths.shape[1]
    per_dest = slots // dests
    cols = u.shape[0] // slots
    chunk = META + FAST
    smem = pl.BlockSpec(memory_space=pltpu.SMEM)
    vmem = pl.BlockSpec(memory_space=pltpu.VMEM)

    def body(*refs):
        pack_kernel(dests, per_dest, cols, *refs)

    main, head = pl.pallas_call(
        body,
        out_shape=(
            jax.ShapeDtypeStruct((dests * chunk, LANES), jnp.float32),
            jax.ShapeDtypeStruct((META, slots), jnp.float32),
        ),
        in_specs=[smem] * 2 + [vmem] * 2,
        out_specs=(vmem, vmem),
        scratch_shapes=[
            pltpu.VMEM((META + (per_dest + 1) * cols, LANES), jnp.float32),
            pltpu.VMEM((slots, LANES), jnp.float32),
        ],
        compiler_params=pltpu.CompilerParams(vmem_limit_bytes=24 << 20),
        cost_estimate=pl.CostEstimate(
            flops=40_000_000, bytes_accessed=8 * dests * chunk * LANES, transcendentals=0
        ),
        name="pack",
    )(slot_of, lengths, u, sums)
    return main.reshape(dests, chunk, LANES), head


def pack_rest(slot_of, lengths, u, dests):
    slots = lengths.shape[1]
    per_dest = slots // dests
    cols = u.shape[0] // slots
    spare = per_dest * cols - FAST

    def body(slot_of, len_ref, u_ref, rest_hbm, stage, sem):
        @pl.loop(0, dests)
        def _(dest):
            def row(r, at):
                s = slot_of[0, dest * per_dest + r]
                first = pl.multiple_of((s >> 3) * (8 * cols) + (s & 7) * 8, 8)
                for j in range(cols // 8):
                    stage[pl.ds(at + 8 * j, 8), :] = u_ref[pl.ds(first + 64 * j, 8), :]
                return at + ((len_ref[0, s] + (LANES - 1)) >> 7)

            lax.fori_loop(0, per_dest, row, jnp.int32(0))
            copy = pltpu.make_async_copy(stage.at[pl.ds(FAST, spare)], rest_hbm.at[dest], sem)
            copy.start()
            copy.wait()

    smem = pl.BlockSpec(memory_space=pltpu.SMEM)
    return pl.pallas_call(
        body,
        out_shape=jax.ShapeDtypeStruct((dests, spare, LANES), jnp.float32),
        in_specs=[smem, smem, pl.BlockSpec(memory_space=pltpu.VMEM)],
        out_specs=pl.BlockSpec(memory_space=pl.ANY),
        scratch_shapes=[
            pltpu.VMEM(((per_dest + 1) * cols, LANES), jnp.float32),
            pltpu.SemaphoreType.DMA,
        ],
        compiler_params=pltpu.CompilerParams(vmem_limit_bytes=16 << 20),
        name="pack_rest",
    )(slot_of, lengths, u)


def score_kernel(members, per_dest, cols, scales, refs):
    (
        main,
        grad_hbm,
        loss_hbm,
        adv_hbm,
        table_ref,
        more_hbm,
        tail,
        grad,
        numbers,
        loss_ref,
        adv_ref,
        more_ref,
        num_sem,
        out_sem,
        small_sem,
    ) = refs
    grad_scale, loss_scale = scales
    width = per_dest * cols
    chunk = META + FAST

    def field(i):
        return jnp.concatenate(
            [main[k * chunk + i : k * chunk + i + 1, :] for k in range(members)], axis=0
        )

    start = lax.rem(lax.axis_index(GY) * per_dest, LANES)
    shift = lax.rem(LANES - start, LANES)
    lengths, reward, sums_p, sums_q = (pltpu.roll(field(i), shift, 1) for i in range(4))
    total = jnp.sum(reward, axis=0, keepdims=True)
    advantage = (members * reward - total) / (members - 1)
    tokens = jnp.sum(field(4), axis=0, keepdims=True)
    scale = grad_scale / tokens
    table_ref[0] = lengths
    table_ref[1] = -advantage * scale
    table_ref[2] = jnp.broadcast_to(scale * -KL, (members, LANES))
    to_scalars = pltpu.make_async_copy(table_ref, numbers, num_sem)
    to_scalars.start()
    loss = (KL * sums_q - advantage * sums_p) * (loss_scale / tokens)
    loss_ref[...] = loss[:, 0:per_dest]
    adv_ref[...] = advantage[:, 0:per_dest]
    most = jnp.max(field(5), axis=0, keepdims=True)
    more_ref[...] = jnp.where(most > FAST, 1, 0)
    small = [
        pltpu.make_async_copy(src, dst, small_sem.at[i])
        for i, (src, dst) in enumerate(
            ((loss_ref, loss_hbm), (adv_ref, adv_hbm), (more_ref, more_hbm))
        )
    ]
    for copy in small:
        copy.start()
    position = sliced_position(cols)
    last = members - 1
    tail[0:chunk, :] = main[last * chunk : (last + 1) * chunk, :]
    to_scalars.wait()

    def out_copy(k):
        part = pl.ds(pl.multiple_of(k * width, width), width)
        return pltpu.make_async_copy(grad.at[part], grad_hbm.at[part], out_sem.at[k])

    def one_member(k, ref, base):
        slope = numbers[2, 0, 0]
        at = base + META
        for r in range(per_dest):
            length = numbers[0, k, r].astype(jnp.int32)
            u = ref[pl.ds(at, cols), :]
            y = jnp.where(position < length, numbers[1, k, r] + slope * u, 0.0)
            first = k * width + r // 8 * (8 * cols) + r % 8
            grad[pl.ds(first, cols, stride=8), :] = y
            at = jnp.minimum(at + ((length + (LANES - 1)) >> 7), base + chunk)
        out_copy(k).start()

    @pl.loop(0, last)
    def _(k):
        one_member(k, main, pl.multiple_of(k * chunk, 8))

    one_member(last, tail, 0)

    for copy in small:
        copy.wait()

    @pl.loop(0, members)
    def _(k):
        out_copy(k).wait()


def score(main, scales, per_dest, cols):
    members, chunk, _ = main.shape
    full = per_dest * cols
    hbm = pl.BlockSpec(memory_space=pl.ANY)
    vmem = pl.BlockSpec(memory_space=pltpu.VMEM)

    def body(*refs):
        score_kernel(members, per_dest, cols, scales, refs)

    small = jax.ShapeDtypeStruct((members, per_dest), jnp.float32)
    return pl.pallas_call(
        body,
        out_shape=(
            jax.ShapeDtypeStruct((members * full, LANES), jnp.float32),
            small,
            small,
            jax.ShapeDtypeStruct((3, members, LANES), jnp.float32),
            jax.ShapeDtypeStruct((1, LANES), jnp.int32),
        ),
        in_specs=[vmem],
        out_specs=(hbm, hbm, hbm, vmem, hbm),
        scratch_shapes=[
            pltpu.VMEM((chunk + cols, LANES), jnp.float32),
            pltpu.VMEM((members * full, LANES), jnp.float32),
            pltpu.SMEM((3, members, LANES), jnp.float32),
            pltpu.VMEM((members, per_dest), jnp.float32),
            pltpu.VMEM((members, per_dest), jnp.float32),
            pltpu.VMEM((1, LANES), jnp.int32),
            pltpu.SemaphoreType.DMA,
            pltpu.SemaphoreType.DMA((members,)),
            pltpu.SemaphoreType.DMA((3,)),
        ],
        compiler_params=pltpu.CompilerParams(vmem_limit_bytes=24 << 20),
        name="score",
    )(main.reshape(members * chunk, LANES))


def finish_kernel(members, per_dest, cols, refs):
    table_hbm, rest_hbm, _, grad_hbm, numbers, rest, grad, sem = refs
    width = per_dest * cols
    spare = width - FAST
    load = pltpu.make_async_copy(table_hbm, numbers, sem.at[0])
    load.start()
    load.wait()
    position = sliced_position(cols)
    row_of = lax.broadcasted_iota(jnp.int32, (cols, LANES), 0)

    @pl.loop(0, members)
    def _(k):
        place = grad_hbm.at[pl.ds(k * width, width)]
        loads = (
            pltpu.make_async_copy(rest_hbm.at[k], rest.at[pl.ds(cols, spare)], sem.at[0]),
            pltpu.make_async_copy(place, grad, sem.at[1]),
        )
        for load in loads:
            load.start()
        for load in loads:
            load.wait()

        def row(r, at):
            length = numbers[0, k, r].astype(jnp.int32)
            end = at + ((length + (LANES - 1)) >> 7)

            @pl.when(end > FAST)
            def _():
                u = rest[pl.ds(at - FAST + cols, cols), :]
                y = jnp.where(position < length, numbers[1, k, r] + numbers[2, 0, 0] * u, 0.0)
                first = (r >> 3) * (8 * cols) + (r & 7)
                old = grad[pl.ds(first, cols, stride=8), :]
                grad[pl.ds(first, cols, stride=8), :] = jnp.where(row_of + at >= FAST, y, old)

            return end

        lax.fori_loop(0, per_dest, row, jnp.int32(0))
        store = pltpu.make_async_copy(grad, place, sem.at[1])
        store.start()
        store.wait()


def finish(grad, rest, table, per_dest, cols):
    members = rest.shape[0]
    full = per_dest * cols
    hbm = pl.BlockSpec(memory_space=pl.ANY)

    def body(*refs):
        finish_kernel(members, per_dest, cols, refs)

    return pl.pallas_call(
        body,
        out_shape=jax.ShapeDtypeStruct(grad.shape, jnp.float32),
        in_specs=[hbm, hbm, hbm],
        out_specs=hbm,
        input_output_aliases={2: 0},
        scratch_shapes=[
            pltpu.SMEM((3, members, LANES), jnp.float32),
            pltpu.VMEM((full - FAST + 2 * cols, LANES), jnp.float32),
            pltpu.VMEM((full, LANES), jnp.float32),
            pltpu.SemaphoreType.DMA((2,)),
        ],
        compiler_params=pltpu.CompilerParams(vmem_limit_bytes=8 << 20),
        name="finish",
    )(table, rest, grad)


def partner(x, step):
    size = lax.axis_size(GX)
    return lax.ppermute(x, GX, [(i, i ^ step) for i in range(size)])


def body(policy_logp, anchor_logp, lengths, rewards, slot_prompt):
    members_dev, slots, seq_slots = policy_logp.shape
    dests = lax.axis_size(GY)
    per_dest = slots // dests
    cols = seq_slots // LANES
    members = members_dev * dests
    samples = members * slots * lax.axis_size(GX)
    scales = (float(samples * seq_slots), float(samples))
    near = [lengths] + [partner(lengths, step) for step in (4, 1, 5)]
    u, sums, slot_of = token_terms(
        *(
            pltpu.with_memory_space_constraint(x, pltpu.HBM)
            for x in (lengths, rewards, slot_prompt, policy_logp[0], anchor_logp[0])
        ),
        dests,
    )
    near = added(near, slot_of)
    main, head = pack(slot_of, lengths, u, sums, dests)
    main = stamp(head, [near, partner(near, 2)], main, per_dest)
    main = lax.all_to_all(main, GY, 0, 0, tiled=True)
    grad, loss, advantage, table, more = score(main, scales, per_dest, cols)

    def the_rest(state):
        grad, _ = state
        rest = pack_rest(slot_of, lengths, u, dests)
        got = lax.all_to_all(rest, GY, 0, 0, tiled=True)
        return finish(grad, got, table, per_dest, cols), jnp.int32(0)

    grad, _ = lax.while_loop(lambda state: state[1] > 0, the_rest, (grad, more[0, 0]))
    grad = (
        grad.reshape(members, per_dest // 8, cols, 8, LANES)
        .transpose(0, 1, 3, 2, 4)
        .reshape(members, per_dest, seq_slots)
    )
    return grad, loss, advantage


def solution(mesh):
    torus = Mesh(mesh.devices.reshape(4, 2, 4, 4), ("gx_0", "gx_1", "gy_0", "gy_1"))
    return jax.shard_map(
        body,
        mesh=torus,
        in_specs=(P(GY, GX, None), P(GY, GX, None), P(GY, GX), P(GY, GX), P(GY, GX)),
        out_specs=(P(None, GX_GY, None), P(None, GX_GY), P(None, GX_GY)),
        check_vma=False,
    )
```

```python
import jax
import jax.numpy as jnp
from jax import lax
from jax.experimental import pallas as pl
from jax.experimental.pallas import tpu as pltpu
from jax.sharding import Mesh
from jax.sharding import PartitionSpec as P

GX_GY = ("gx_0", "gx_1", "gy_0", "gy_1")
GY = ("gy_0", "gy_1")
GX = ("gx_0", "gx_1")

KL = 0.1
LANES = 128
META = 8
FAST = 432


def sliced_position(cols):
    row = lax.broadcasted_iota(jnp.int32, (cols, LANES), 0)
    return row * LANES + lax.broadcasted_iota(jnp.int32, (cols, LANES), 1)


SPAN = LANES // 4
LEN, SUM_P, REWARD, SUM_Q = (i * SPAN for i in range(4))
STEPS = 16


def token_kernel(
    dests,
    small_hbm,
    policy_hbm,
    anchor_hbm,
    u_ref,
    sums_ref,
    slot_hbm,
    policy,
    anchor,
    parts,
    len_ref,
    reward_ref,
    prompt_ref,
    slot_of,
    sem,
    small_sem,
):
    slots, width = policy.shape
    rows = slots // STEPS
    cols = width // LANES
    per_dest = slots // dests

    def loads(step):
        part = pl.ds(pl.multiple_of(step * rows, rows), rows)
        return (
            pltpu.make_async_copy(policy_hbm.at[part], policy.at[part], sem.at[0, step]),
            pltpu.make_async_copy(anchor_hbm.at[part], anchor.at[part], sem.at[1, step]),
        )

    small = [
        pltpu.make_async_copy(src, dst, small_sem.at[i])
        for i, (src, dst) in enumerate(zip(small_hbm, (prompt_ref, len_ref, reward_ref)))
    ]
    for load in small:
        load.start()
    for step in range(STEPS):
        for load in loads(step):
            load.start()
    for load in small:
        load.wait()

    def invert(s, carry):
        slot_of[0, prompt_ref[0, s] & (slots - 1)] = s
        return carry

    lax.fori_loop(0, slots, invert, 0, unroll=16)
    inverse = pltpu.make_async_copy(slot_of, slot_hbm, small_sem.at[3])
    inverse.start()
    lane = lax.broadcasted_iota(jnp.int32, (8, LANES), 1)
    sub = lax.broadcasted_iota(jnp.int32, (8, LANES), 0)

    @pl.loop(0, STEPS)
    def _(step):
        for load in loads(step):
            load.wait()

        @pl.loop(0, rows // 8)
        def _(group):
            first = pl.multiple_of(step * rows + group * 8, 8)
            length = jnp.full((8, LANES), len_ref[0, first], jnp.int32)
            reward = jnp.full((8, LANES), reward_ref[0, first], jnp.int32)
            for i in range(1, 8):
                length = jnp.where(sub == i, len_ref[0, first + i], length)
                reward = jnp.where(sub == i, reward_ref[0, first + i], reward)
            sums_ref[pl.ds(first, 8), :] = jnp.where(lane < REWARD, length, reward).astype(
                jnp.float32
            )
            behind = lane - length
            sums_p = [jnp.zeros((8, LANES), jnp.float32)] * 4
            sums_q = [jnp.zeros((8, LANES), jnp.float32)] * 4
            for c in range(cols):
                at = (pl.ds(first, 8), pl.ds(c * LANES, LANES))
                a = policy[at]
                d = anchor[at] - a
                valid = behind < -c * LANES
                u = jnp.exp(d) - 1.0
                u_ref[pl.ds(first * cols + c // 8 * 64 + c % 8, 8, stride=8), :] = u
                sums_q[c % 4] = sums_q[c % 4] + jnp.where(valid, u - d, 0.0)
                sums_p[c % 4] = sums_p[c % 4] + jnp.where(valid, a, 0.0)
            parts[0, pl.ds(first, 8), :] = (sums_p[0] + sums_p[1]) + (sums_p[2] + sums_p[3])
            parts[1, pl.ds(first, 8), :] = (sums_q[0] + sums_q[1]) + (sums_q[2] + sums_q[3])

    inverse.wait()
    lane = lax.broadcasted_iota(jnp.int32, (slots, LANES), 1)
    p, q = (x + pltpu.roll(x, 2 * SPAN, 1) for x in (parts[0], parts[1]))
    both = jnp.where(lane < REWARD, p, q)
    both = both + pltpu.roll(both, SPAN, 1)
    summed = (lane >= SUM_P) & (lane < REWARD) | (lane >= SUM_Q)
    sums_ref[...] = jnp.where(summed, both, sums_ref[...])


def token_terms(lengths, rewards, prompts, policy, anchor, dests):
    slots, width = policy.shape
    vmem = pl.BlockSpec(memory_space=pltpu.VMEM)
    hbm = pl.BlockSpec(memory_space=pl.ANY)

    def body(*refs):
        token_kernel(dests, refs[:3], *refs[3:])

    return pl.pallas_call(
        body,
        out_shape=(
            jax.ShapeDtypeStruct((slots * width // LANES, LANES), jnp.float32),
            jax.ShapeDtypeStruct((slots, LANES), jnp.float32),
            jax.ShapeDtypeStruct((1, slots), jnp.int32),
        ),
        in_specs=[hbm] * 5,
        out_specs=(vmem, vmem, hbm),
        scratch_shapes=[
            pltpu.VMEM((slots, width), jnp.float32),
            pltpu.VMEM((slots, width), jnp.float32),
            pltpu.VMEM((2, slots, LANES), jnp.float32),
            pltpu.SMEM((1, slots), jnp.int32),
            pltpu.SMEM((1, slots), jnp.int32),
            pltpu.SMEM((1, slots), jnp.int32),
            pltpu.SMEM((1, slots), jnp.int32),
            pltpu.SemaphoreType.DMA((2, STEPS)),
            pltpu.SemaphoreType.DMA((4,)),
        ],
        compiler_params=pltpu.CompilerParams(vmem_limit_bytes=24 << 20),
        cost_estimate=pl.CostEstimate(
            flops=40_000_000, bytes_accessed=12 * slots * width, transcendentals=slots * width
        ),
        name="token_terms",
    )(prompts, lengths, rewards, policy, anchor)


def pack_kernel(
    dests,
    per_dest,
    cols,
    slot_of,
    len_ref,
    u_ref,
    sums_ref,
    main,
    head_ref,
    stage,
    in_order,
):
    slots = dests * per_dest
    chunk = META + FAST
    last = dests - 1

    def one_dest(dest, most, ref, base):
        def row(r, at):
            p = dest * per_dest + r
            s = slot_of[0, p]
            first = pl.multiple_of((s >> 3) * (8 * cols) + (s & 7) * 8, 8)
            for j in range(cols // 8):
                ref[pl.ds(at + 8 * j, 8), :] = u_ref[pl.ds(first + 64 * j, 8), :]
            in_order[pl.ds(p, 1), :] = sums_ref[pl.ds(s, 1), :]
            return at + ((len_ref[0, s] + (LANES - 1)) >> 7)

        end = lax.fori_loop(0, per_dest, row, base + META, unroll=4)
        return jnp.maximum(most, end - base - META)

    def in_place(dest, most):
        return one_dest(dest, most, main, pl.multiple_of(dest * chunk, 8))

    most = lax.fori_loop(0, last, in_place, jnp.int32(0))
    most = one_dest(last, most, stage, 0)
    main[last * chunk + META : (last + 1) * chunk, :] = stage[META:chunk, :]

    sub = lax.broadcasted_iota(jnp.int32, (8, LANES), 0)
    lane = lax.broadcasted_iota(jnp.int32, (8, LANES), 1)
    pick = jnp.where((sub == 0) & (lane == LEN), 1.0, 0.0)
    pick = jnp.where((sub == 1) & (lane == REWARD), 0.25, pick)
    pick = jnp.where((sub == 2) & (lane >= SUM_P) & (lane < REWARD), 1.0, pick)
    pick = jnp.where((sub == 3) & (lane >= SUM_Q), 1.0, pick)
    head = lax.dot_general(
        pick,
        in_order[...],
        (((1,), (1,)), ((), ())),
        precision=lax.Precision.HIGHEST,
        preferred_element_type=jnp.float32,
    )
    sub = lax.broadcasted_iota(jnp.int32, (8, slots), 0)
    head_ref[...] = jnp.where(sub == 5, most.astype(jnp.float32), head)


def stamp_kernel(dests, per_dest, head, counts, _, main, tile, sem):
    sub = lax.broadcasted_iota(jnp.int32, (8, LANES), 0)
    count = jnp.sum(sum(c[...] for c in counts).astype(jnp.float32), axis=1, keepdims=True)
    halves = head.shape[1] // LANES
    for half in range(halves):
        tile[half] = jnp.where(sub == 4, count, head[:, half * LANES : (half + 1) * LANES])
    copies = [
        pltpu.make_async_copy(
            tile.at[dest * per_dest // LANES], main.at[dest, pl.ds(0, META)], sem.at[dest]
        )
        for dest in range(dests)
    ]
    for copy in copies:
        copy.start()
    for copy in copies:
        copy.wait()


def stamp(head, counts, main, per_dest):
    dests = main.shape[0]
    vmem = pl.BlockSpec(memory_space=pltpu.VMEM)
    place = pl.BlockSpec(memory_space=pl.ANY)

    def body(head, *refs):
        stamp_kernel(dests, per_dest, head, refs[: len(counts)], *refs[len(counts) :])

    return pl.pallas_call(
        body,
        out_shape=jax.ShapeDtypeStruct(main.shape, jnp.float32),
        in_specs=[vmem] * (1 + len(counts)) + [place],
        out_specs=place,
        input_output_aliases={1 + len(counts): 0},
        scratch_shapes=[
            pltpu.VMEM((head.shape[1] // LANES, META, LANES), jnp.float32),
            pltpu.SemaphoreType.DMA((dests,)),
        ],
        compiler_params=pltpu.CompilerParams(vmem_limit_bytes=4 << 20),
        name="stamp",
    )(head, *counts, main)


def added(parts, after):
    def body(*refs):
        refs[-1][...] = sum(x[...] for x in refs[:-2])

    vmem = pl.BlockSpec(memory_space=pltpu.VMEM)
    return pl.pallas_call(
        body,
        out_shape=jax.ShapeDtypeStruct(parts[0].shape, parts[0].dtype),
        in_specs=[vmem] * len(parts) + [pl.BlockSpec(memory_space=pl.ANY)],
        out_specs=vmem,
        compiler_params=pltpu.CompilerParams(vmem_limit_bytes=4 << 20),
        name="added",
    )(*parts, after)


def pack(slot_of, lengths, u, sums, dests):
    slots = lengths.shape[1]
    per_dest = slots // dests
    cols = u.shape[0] // slots
    chunk = META + FAST
    smem = pl.BlockSpec(memory_space=pltpu.SMEM)
    vmem = pl.BlockSpec(memory_space=pltpu.VMEM)

    def body(*refs):
        pack_kernel(dests, per_dest, cols, *refs)

    main, head = pl.pallas_call(
        body,
        out_shape=(
            jax.ShapeDtypeStruct((dests * chunk, LANES), jnp.float32),
            jax.ShapeDtypeStruct((META, slots), jnp.float32),
        ),
        in_specs=[smem] * 2 + [vmem] * 2,
        out_specs=(vmem, vmem),
        scratch_shapes=[
            pltpu.VMEM((META + (per_dest + 1) * cols, LANES), jnp.float32),
            pltpu.VMEM((slots, LANES), jnp.float32),
        ],
        compiler_params=pltpu.CompilerParams(vmem_limit_bytes=24 << 20),
        cost_estimate=pl.CostEstimate(
            flops=40_000_000, bytes_accessed=8 * dests * chunk * LANES, transcendentals=0
        ),
        name="pack",
    )(slot_of, lengths, u, sums)
    return main.reshape(dests, chunk, LANES), head


def pack_rest(slot_of, lengths, u, dests):
    slots = lengths.shape[1]
    per_dest = slots // dests
    cols = u.shape[0] // slots
    spare = per_dest * cols - FAST

    def body(slot_of, len_ref, u_ref, rest_hbm, stage, sem):
        @pl.loop(0, dests)
        def _(dest):
            def row(r, at):
                s = slot_of[0, dest * per_dest + r]
                first = pl.multiple_of((s >> 3) * (8 * cols) + (s & 7) * 8, 8)
                for j in range(cols // 8):
                    stage[pl.ds(at + 8 * j, 8), :] = u_ref[pl.ds(first + 64 * j, 8), :]
                return at + ((len_ref[0, s] + (LANES - 1)) >> 7)

            lax.fori_loop(0, per_dest, row, jnp.int32(0))
            copy = pltpu.make_async_copy(stage.at[pl.ds(FAST, spare)], rest_hbm.at[dest], sem)
            copy.start()
            copy.wait()

    smem = pl.BlockSpec(memory_space=pltpu.SMEM)
    return pl.pallas_call(
        body,
        out_shape=jax.ShapeDtypeStruct((dests, spare, LANES), jnp.float32),
        in_specs=[smem, smem, pl.BlockSpec(memory_space=pltpu.VMEM)],
        out_specs=pl.BlockSpec(memory_space=pl.ANY),
        scratch_shapes=[
            pltpu.VMEM(((per_dest + 1) * cols, LANES), jnp.float32),
            pltpu.SemaphoreType.DMA,
        ],
        compiler_params=pltpu.CompilerParams(vmem_limit_bytes=16 << 20),
        name="pack_rest",
    )(slot_of, lengths, u)


def score_kernel(members, per_dest, cols, scales, refs):
    (
        main,
        grad_hbm,
        loss_hbm,
        adv_hbm,
        table_ref,
        more_hbm,
        tail,
        grad,
        numbers,
        loss_ref,
        adv_ref,
        more_ref,
        num_sem,
        out_sem,
        small_sem,
    ) = refs
    grad_scale, loss_scale = scales
    width = per_dest * cols
    chunk = META + FAST

    def field(i):
        return jnp.concatenate(
            [main[k * chunk + i : k * chunk + i + 1, :] for k in range(members)], axis=0
        )

    start = lax.rem(lax.axis_index(GY) * per_dest, LANES)
    shift = lax.rem(LANES - start, LANES)
    lengths, reward, sums_p, sums_q = (pltpu.roll(field(i), shift, 1) for i in range(4))
    total = jnp.sum(reward, axis=0, keepdims=True)
    advantage = (members * reward - total) / (members - 1)
    tokens = jnp.sum(field(4), axis=0, keepdims=True)
    scale = grad_scale / tokens
    table_ref[0] = lengths
    table_ref[1] = -advantage * scale
    table_ref[2] = jnp.broadcast_to(scale * -KL, (members, LANES))
    to_scalars = pltpu.make_async_copy(table_ref, numbers, num_sem)
    to_scalars.start()
    loss = (KL * sums_q - advantage * sums_p) * (loss_scale / tokens)
    loss_ref[...] = loss[:, 0:per_dest]
    adv_ref[...] = advantage[:, 0:per_dest]
    most = jnp.max(field(5), axis=0, keepdims=True)
    more_ref[...] = jnp.where(most > FAST, 1, 0)
    small = [
        pltpu.make_async_copy(src, dst, small_sem.at[i])
        for i, (src, dst) in enumerate(
            ((loss_ref, loss_hbm), (adv_ref, adv_hbm), (more_ref, more_hbm))
        )
    ]
    for copy in small:
        copy.start()
    position = sliced_position(cols)
    last = members - 1
    tail[0:chunk, :] = main[last * chunk : (last + 1) * chunk, :]
    to_scalars.wait()

    def out_copy(k):
        part = pl.ds(pl.multiple_of(k * width, width), width)
        return pltpu.make_async_copy(grad.at[part], grad_hbm.at[part], out_sem.at[k])

    def one_member(k, ref, base):
        slope = numbers[2, 0, 0]
        at = base + META
        for r in range(per_dest):
            length = numbers[0, k, r].astype(jnp.int32)
            u = ref[pl.ds(at, cols), :]
            y = jnp.where(position < length, numbers[1, k, r] + slope * u, 0.0)
            first = k * width + r // 8 * (8 * cols) + r % 8
            grad[pl.ds(first, cols, stride=8), :] = y
            at = jnp.minimum(at + ((length + (LANES - 1)) >> 7), base + chunk)
        out_copy(k).start()

    @pl.loop(0, last)
    def _(k):
        one_member(k, main, pl.multiple_of(k * chunk, 8))

    one_member(last, tail, 0)

    for copy in small:
        copy.wait()

    @pl.loop(0, members)
    def _(k):
        out_copy(k).wait()


def score(main, scales, per_dest, cols):
    members, chunk, _ = main.shape
    full = per_dest * cols
    hbm = pl.BlockSpec(memory_space=pl.ANY)
    vmem = pl.BlockSpec(memory_space=pltpu.VMEM)

    def body(*refs):
        score_kernel(members, per_dest, cols, scales, refs)

    small = jax.ShapeDtypeStruct((members, per_dest), jnp.float32)
    return pl.pallas_call(
        body,
        out_shape=(
            jax.ShapeDtypeStruct((members * full, LANES), jnp.float32),
            small,
            small,
            jax.ShapeDtypeStruct((3, members, LANES), jnp.float32),
            jax.ShapeDtypeStruct((1, LANES), jnp.int32),
        ),
        in_specs=[vmem],
        out_specs=(hbm, hbm, hbm, vmem, hbm),
        scratch_shapes=[
            pltpu.VMEM((chunk + cols, LANES), jnp.float32),
            pltpu.VMEM((members * full, LANES), jnp.float32),
            pltpu.SMEM((3, members, LANES), jnp.float32),
            pltpu.VMEM((members, per_dest), jnp.float32),
            pltpu.VMEM((members, per_dest), jnp.float32),
            pltpu.VMEM((1, LANES), jnp.int32),
            pltpu.SemaphoreType.DMA,
            pltpu.SemaphoreType.DMA((members,)),
            pltpu.SemaphoreType.DMA((3,)),
        ],
        compiler_params=pltpu.CompilerParams(vmem_limit_bytes=24 << 20),
        name="score",
    )(main.reshape(members * chunk, LANES))


def finish_kernel(members, per_dest, cols, refs):
    table_hbm, rest_hbm, _, grad_hbm, numbers, rest, grad, sem = refs
    width = per_dest * cols
    spare = width - FAST
    load = pltpu.make_async_copy(table_hbm, numbers, sem.at[0])
    load.start()
    load.wait()
    position = sliced_position(cols)
    row_of = lax.broadcasted_iota(jnp.int32, (cols, LANES), 0)

    @pl.loop(0, members)
    def _(k):
        place = grad_hbm.at[pl.ds(k * width, width)]
        loads = (
            pltpu.make_async_copy(rest_hbm.at[k], rest.at[pl.ds(cols, spare)], sem.at[0]),
            pltpu.make_async_copy(place, grad, sem.at[1]),
        )
        for load in loads:
            load.start()
        for load in loads:
            load.wait()

        def row(r, at):
            length = numbers[0, k, r].astype(jnp.int32)
            end = at + ((length + (LANES - 1)) >> 7)

            @pl.when(end > FAST)
            def _():
                u = rest[pl.ds(at - FAST + cols, cols), :]
                y = jnp.where(position < length, numbers[1, k, r] + numbers[2, 0, 0] * u, 0.0)
                first = (r >> 3) * (8 * cols) + (r & 7)
                old = grad[pl.ds(first, cols, stride=8), :]
                grad[pl.ds(first, cols, stride=8), :] = jnp.where(row_of + at >= FAST, y, old)

            return end

        lax.fori_loop(0, per_dest, row, jnp.int32(0))
        store = pltpu.make_async_copy(grad, place, sem.at[1])
        store.start()
        store.wait()


def finish(grad, rest, table, per_dest, cols):
    members = rest.shape[0]
    full = per_dest * cols
    hbm = pl.BlockSpec(memory_space=pl.ANY)

    def body(*refs):
        finish_kernel(members, per_dest, cols, refs)

    return pl.pallas_call(
        body,
        out_shape=jax.ShapeDtypeStruct(grad.shape, jnp.float32),
        in_specs=[hbm, hbm, hbm],
        out_specs=hbm,
        input_output_aliases={2: 0},
        scratch_shapes=[
            pltpu.SMEM((3, members, LANES), jnp.float32),
            pltpu.VMEM((full - FAST + 2 * cols, LANES), jnp.float32),
            pltpu.VMEM((full, LANES), jnp.float32),
            pltpu.SemaphoreType.DMA((2,)),
        ],
        compiler_params=pltpu.CompilerParams(vmem_limit_bytes=8 << 20),
        name="finish",
    )(table, rest, grad)


def partner(x, step):
    size = lax.axis_size(GX)
    return lax.ppermute(x, GX, [(i, i ^ step) for i in range(size)])


def body(policy_logp, anchor_logp, lengths, rewards, slot_prompt):
    members_dev, slots, seq_slots = policy_logp.shape
    dests = lax.axis_size(GY)
    per_dest = slots // dests
    cols = seq_slots // LANES
    members = members_dev * dests
    samples = members * slots * lax.axis_size(GX)
    scales = (float(samples * seq_slots), float(samples))
    near = [lengths] + [partner(lengths, step) for step in (5, 4, 1)]
    u, sums, slot_of = token_terms(
        *(
            pltpu.with_memory_space_constraint(x, pltpu.HBM)
            for x in (lengths, rewards, slot_prompt, policy_logp[0], anchor_logp[0])
        ),
        dests,
    )
    near = added(near, slot_of)
    main, head = pack(slot_of, lengths, u, sums, dests)
    main = stamp(head, [near, partner(near, 2)], main, per_dest)
    main = lax.all_to_all(main, GY, 0, 0, tiled=True)
    grad, loss, advantage, table, more = score(main, scales, per_dest, cols)

    def the_rest(state):
        grad, _ = state
        rest = pack_rest(slot_of, lengths, u, dests)
        got = lax.all_to_all(rest, GY, 0, 0, tiled=True)
        return finish(grad, got, table, per_dest, cols), jnp.int32(0)

    grad, _ = lax.while_loop(lambda state: state[1] > 0, the_rest, (grad, more[0, 0]))
    grad = (
        grad.reshape(members, per_dest // 8, cols, 8, LANES)
        .transpose(0, 1, 3, 2, 4)
        .reshape(members, per_dest, seq_slots)
    )
    return grad, loss, advantage


def solution(mesh):
    torus = Mesh(mesh.devices.reshape(4, 2, 4, 4), ("gx_0", "gx_1", "gy_0", "gy_1"))
    return jax.shard_map(
        body,
        mesh=torus,
        in_specs=(P(GY, GX, None), P(GY, GX, None), P(GY, GX), P(GY, GX), P(GY, GX)),
        out_specs=(P(None, GX_GY, None), P(None, GX_GY), P(None, GX_GY)),
        check_vma=False,
    )
```

```python
import jax
import jax.numpy as jnp
from jax import lax
from jax.experimental import pallas as pl
from jax.experimental.pallas import tpu as pltpu
from jax.sharding import Mesh
from jax.sharding import PartitionSpec as P

GX_GY = ("gx_0", "gx_1", "gy_0", "gy_1")
GY = ("gy_0", "gy_1")
GX = ("gx_0", "gx_1")

KL = 0.1
LANES = 128
META = 8
FAST = 432


def sliced_position(cols):
    row = lax.broadcasted_iota(jnp.int32, (cols, LANES), 0)
    return row * LANES + lax.broadcasted_iota(jnp.int32, (cols, LANES), 1)


LEAST = 512
SPAN = LANES // 4
LEN, SUM_P, REWARD, SUM_Q = (i * SPAN for i in range(4))
STEPS = 16


def token_kernel(
    dests,
    small_hbm,
    policy_hbm,
    anchor_hbm,
    u_ref,
    sums_ref,
    slot_hbm,
    policy,
    anchor,
    parts,
    len_ref,
    reward_ref,
    prompt_ref,
    slot_of,
    sem,
    small_sem,
):
    slots, width = policy.shape
    rows = slots // STEPS
    cols = width // LANES
    per_dest = slots // dests

    def loads(step):
        part = pl.ds(pl.multiple_of(step * rows, rows), rows)
        return (
            pltpu.make_async_copy(policy_hbm.at[part], policy.at[part], sem.at[0, step]),
            pltpu.make_async_copy(anchor_hbm.at[part], anchor.at[part], sem.at[1, step]),
        )

    small = [
        pltpu.make_async_copy(src, dst, small_sem.at[i])
        for i, (src, dst) in enumerate(zip(small_hbm, (prompt_ref, len_ref, reward_ref)))
    ]
    for load in small:
        load.start()
    for step in range(STEPS):
        for load in loads(step):
            load.start()
    for load in small:
        load.wait()

    def invert(s, carry):
        slot_of[0, prompt_ref[0, s] & (slots - 1)] = s
        return carry

    lax.fori_loop(0, slots, invert, 0, unroll=16)
    inverse = pltpu.make_async_copy(slot_of, slot_hbm, small_sem.at[3])
    inverse.start()
    lane = lax.broadcasted_iota(jnp.int32, (8, LANES), 1)
    sub = lax.broadcasted_iota(jnp.int32, (8, LANES), 0)

    @pl.loop(0, STEPS)
    def _(step):
        for load in loads(step):
            load.wait()

        @pl.loop(0, rows // 8)
        def _(group):
            first = pl.multiple_of(step * rows + group * 8, 8)
            length = jnp.full((8, LANES), len_ref[0, first], jnp.int32)
            reward = jnp.full((8, LANES), reward_ref[0, first], jnp.int32)
            for i in range(1, 8):
                length = jnp.where(sub == i, len_ref[0, first + i], length)
                reward = jnp.where(sub == i, reward_ref[0, first + i], reward)
            sums_ref[pl.ds(first, 8), :] = jnp.where(lane < REWARD, length, reward).astype(
                jnp.float32
            )
            behind = lane - length
            sums_p = [jnp.zeros((8, LANES), jnp.float32)] * 4
            sums_q = [jnp.zeros((8, LANES), jnp.float32)] * 4
            for c in range(cols):
                at = (pl.ds(first, 8), pl.ds(c * LANES, LANES))
                a = policy[at]
                d = anchor[at] - a
                u = jnp.exp(d) - 1.0
                u_ref[pl.ds(first * cols + c // 8 * 64 + c % 8, 8, stride=8), :] = u
                q = u - d
                if (c + 1) * LANES > LEAST:
                    valid = behind < -c * LANES
                    q = jnp.where(valid, q, 0.0)
                    a = jnp.where(valid, a, 0.0)
                sums_q[c % 4] = sums_q[c % 4] + q
                sums_p[c % 4] = sums_p[c % 4] + a
            parts[0, pl.ds(first, 8), :] = (sums_p[0] + sums_p[1]) + (sums_p[2] + sums_p[3])
            parts[1, pl.ds(first, 8), :] = (sums_q[0] + sums_q[1]) + (sums_q[2] + sums_q[3])

    inverse.wait()
    lane = lax.broadcasted_iota(jnp.int32, (slots, LANES), 1)
    p, q = (x + pltpu.roll(x, 2 * SPAN, 1) for x in (parts[0], parts[1]))
    both = jnp.where(lane < REWARD, p, q)
    both = both + pltpu.roll(both, SPAN, 1)
    summed = (lane >= SUM_P) & (lane < REWARD) | (lane >= SUM_Q)
    sums_ref[...] = jnp.where(summed, both, sums_ref[...])


def token_terms(lengths, rewards, prompts, policy, anchor, dests):
    slots, width = policy.shape
    vmem = pl.BlockSpec(memory_space=pltpu.VMEM)
    hbm = pl.BlockSpec(memory_space=pl.ANY)

    def body(*refs):
        token_kernel(dests, refs[:3], *refs[3:])

    return pl.pallas_call(
        body,
        out_shape=(
            jax.ShapeDtypeStruct((slots * width // LANES, LANES), jnp.float32),
            jax.ShapeDtypeStruct((slots, LANES), jnp.float32),
            jax.ShapeDtypeStruct((1, slots), jnp.int32),
        ),
        in_specs=[hbm] * 5,
        out_specs=(vmem, vmem, hbm),
        scratch_shapes=[
            pltpu.VMEM((slots, width), jnp.float32),
            pltpu.VMEM((slots, width), jnp.float32),
            pltpu.VMEM((2, slots, LANES), jnp.float32),
            pltpu.SMEM((1, slots), jnp.int32),
            pltpu.SMEM((1, slots), jnp.int32),
            pltpu.SMEM((1, slots), jnp.int32),
            pltpu.SMEM((1, slots), jnp.int32),
            pltpu.SemaphoreType.DMA((2, STEPS)),
            pltpu.SemaphoreType.DMA((4,)),
        ],
        compiler_params=pltpu.CompilerParams(vmem_limit_bytes=24 << 20),
        cost_estimate=pl.CostEstimate(
            flops=40_000_000, bytes_accessed=12 * slots * width, transcendentals=slots * width
        ),
        name="token_terms",
    )(prompts, lengths, rewards, policy, anchor)


def pack_kernel(
    dests,
    per_dest,
    cols,
    slot_of,
    len_ref,
    u_ref,
    sums_ref,
    main,
    head_ref,
    stage,
    in_order,
):
    slots = dests * per_dest
    chunk = META + FAST
    last = dests - 1

    def one_dest(dest, most, ref, base):
        def row(r, at):
            p = dest * per_dest + r
            s = slot_of[0, p]
            first = pl.multiple_of((s >> 3) * (8 * cols) + (s & 7) * 8, 8)
            for j in range(cols // 8):
                ref[pl.ds(at + 8 * j, 8), :] = u_ref[pl.ds(first + 64 * j, 8), :]
            in_order[pl.ds(p, 1), :] = sums_ref[pl.ds(s, 1), :]
            return at + ((len_ref[0, s] + (LANES - 1)) >> 7)

        end = lax.fori_loop(0, per_dest, row, base + META, unroll=4)
        return jnp.maximum(most, end - base - META)

    def in_place(dest, most):
        return one_dest(dest, most, main, pl.multiple_of(dest * chunk, 8))

    most = lax.fori_loop(0, last, in_place, jnp.int32(0))
    most = one_dest(last, most, stage, 0)
    main[last * chunk + META : (last + 1) * chunk, :] = stage[META:chunk, :]

    sub = lax.broadcasted_iota(jnp.int32, (8, LANES), 0)
    lane = lax.broadcasted_iota(jnp.int32, (8, LANES), 1)
    pick = jnp.where((sub == 0) & (lane == LEN), 1.0, 0.0)
    pick = jnp.where((sub == 1) & (lane == REWARD), 0.25, pick)
    pick = jnp.where((sub == 2) & (lane >= SUM_P) & (lane < REWARD), 1.0, pick)
    pick = jnp.where((sub == 3) & (lane >= SUM_Q), 1.0, pick)
    head = lax.dot_general(
        pick,
        in_order[...],
        (((1,), (1,)), ((), ())),
        precision=lax.Precision.HIGHEST,
        preferred_element_type=jnp.float32,
    )
    sub = lax.broadcasted_iota(jnp.int32, (8, slots), 0)
    head_ref[...] = jnp.where(sub == 5, most.astype(jnp.float32), head)


def stamp_kernel(dests, per_dest, head, counts, _, main, tile, sem):
    sub = lax.broadcasted_iota(jnp.int32, (8, LANES), 0)
    count = jnp.sum(sum(c[...] for c in counts).astype(jnp.float32), axis=1, keepdims=True)
    halves = head.shape[1] // LANES
    for half in range(halves):
        tile[half] = jnp.where(sub == 4, count, head[:, half * LANES : (half + 1) * LANES])
    copies = [
        pltpu.make_async_copy(
            tile.at[dest * per_dest // LANES], main.at[dest, pl.ds(0, META)], sem.at[dest]
        )
        for dest in range(dests)
    ]
    for copy in copies:
        copy.start()
    for copy in copies:
        copy.wait()


def stamp(head, counts, main, per_dest):
    dests = main.shape[0]
    vmem = pl.BlockSpec(memory_space=pltpu.VMEM)
    place = pl.BlockSpec(memory_space=pl.ANY)

    def body(head, *refs):
        stamp_kernel(dests, per_dest, head, refs[: len(counts)], *refs[len(counts) :])

    return pl.pallas_call(
        body,
        out_shape=jax.ShapeDtypeStruct(main.shape, jnp.float32),
        in_specs=[vmem] * (1 + len(counts)) + [place],
        out_specs=place,
        input_output_aliases={1 + len(counts): 0},
        scratch_shapes=[
            pltpu.VMEM((head.shape[1] // LANES, META, LANES), jnp.float32),
            pltpu.SemaphoreType.DMA((dests,)),
        ],
        compiler_params=pltpu.CompilerParams(vmem_limit_bytes=4 << 20),
        name="stamp",
    )(head, *counts, main)


def added(parts, after):
    def body(*refs):
        refs[-1][...] = sum(x[...] for x in refs[:-2])

    vmem = pl.BlockSpec(memory_space=pltpu.VMEM)
    return pl.pallas_call(
        body,
        out_shape=jax.ShapeDtypeStruct(parts[0].shape, parts[0].dtype),
        in_specs=[vmem] * len(parts) + [pl.BlockSpec(memory_space=pl.ANY)],
        out_specs=vmem,
        compiler_params=pltpu.CompilerParams(vmem_limit_bytes=4 << 20),
        name="added",
    )(*parts, after)


def pack(slot_of, lengths, u, sums, dests):
    slots = lengths.shape[1]
    per_dest = slots // dests
    cols = u.shape[0] // slots
    chunk = META + FAST
    smem = pl.BlockSpec(memory_space=pltpu.SMEM)
    vmem = pl.BlockSpec(memory_space=pltpu.VMEM)

    def body(*refs):
        pack_kernel(dests, per_dest, cols, *refs)

    main, head = pl.pallas_call(
        body,
        out_shape=(
            jax.ShapeDtypeStruct((dests * chunk, LANES), jnp.float32),
            jax.ShapeDtypeStruct((META, slots), jnp.float32),
        ),
        in_specs=[smem] * 2 + [vmem] * 2,
        out_specs=(vmem, vmem),
        scratch_shapes=[
            pltpu.VMEM((META + (per_dest + 1) * cols, LANES), jnp.float32),
            pltpu.VMEM((slots, LANES), jnp.float32),
        ],
        compiler_params=pltpu.CompilerParams(vmem_limit_bytes=24 << 20),
        cost_estimate=pl.CostEstimate(
            flops=40_000_000, bytes_accessed=8 * dests * chunk * LANES, transcendentals=0
        ),
        name="pack",
    )(slot_of, lengths, u, sums)
    return main.reshape(dests, chunk, LANES), head


def pack_rest(slot_of, lengths, u, dests):
    slots = lengths.shape[1]
    per_dest = slots // dests
    cols = u.shape[0] // slots
    spare = per_dest * cols - FAST

    def body(slot_of, len_ref, u_ref, rest_hbm, stage, sem):
        @pl.loop(0, dests)
        def _(dest):
            def row(r, at):
                s = slot_of[0, dest * per_dest + r]
                first = pl.multiple_of((s >> 3) * (8 * cols) + (s & 7) * 8, 8)
                for j in range(cols // 8):
                    stage[pl.ds(at + 8 * j, 8), :] = u_ref[pl.ds(first + 64 * j, 8), :]
                return at + ((len_ref[0, s] + (LANES - 1)) >> 7)

            lax.fori_loop(0, per_dest, row, jnp.int32(0))
            copy = pltpu.make_async_copy(stage.at[pl.ds(FAST, spare)], rest_hbm.at[dest], sem)
            copy.start()
            copy.wait()

    smem = pl.BlockSpec(memory_space=pltpu.SMEM)
    return pl.pallas_call(
        body,
        out_shape=jax.ShapeDtypeStruct((dests, spare, LANES), jnp.float32),
        in_specs=[smem, smem, pl.BlockSpec(memory_space=pltpu.VMEM)],
        out_specs=pl.BlockSpec(memory_space=pl.ANY),
        scratch_shapes=[
            pltpu.VMEM(((per_dest + 1) * cols, LANES), jnp.float32),
            pltpu.SemaphoreType.DMA,
        ],
        compiler_params=pltpu.CompilerParams(vmem_limit_bytes=16 << 20),
        name="pack_rest",
    )(slot_of, lengths, u)


def score_kernel(members, per_dest, cols, scales, refs):
    (
        main,
        grad_hbm,
        loss_hbm,
        adv_hbm,
        table_ref,
        more_hbm,
        tail,
        grad,
        numbers,
        loss_ref,
        adv_ref,
        more_ref,
        num_sem,
        out_sem,
        small_sem,
    ) = refs
    grad_scale, loss_scale = scales
    width = per_dest * cols
    chunk = META + FAST

    def field(i):
        return jnp.concatenate(
            [main[k * chunk + i : k * chunk + i + 1, :] for k in range(members)], axis=0
        )

    start = lax.rem(lax.axis_index(GY) * per_dest, LANES)
    shift = lax.rem(LANES - start, LANES)
    lengths, reward, sums_p, sums_q = (pltpu.roll(field(i), shift, 1) for i in range(4))
    total = jnp.sum(reward, axis=0, keepdims=True)
    advantage = (members * reward - total) / (members - 1)
    tokens = jnp.sum(field(4), axis=0, keepdims=True)
    scale = grad_scale / tokens
    table_ref[0] = lengths
    table_ref[1] = -advantage * scale
    table_ref[2] = jnp.broadcast_to(scale * -KL, (members, LANES))
    to_scalars = pltpu.make_async_copy(table_ref, numbers, num_sem)
    to_scalars.start()
    loss = (KL * sums_q - advantage * sums_p) * (loss_scale / tokens)
    loss_ref[...] = loss[:, 0:per_dest]
    adv_ref[...] = advantage[:, 0:per_dest]
    most = jnp.max(field(5), axis=0, keepdims=True)
    more_ref[...] = jnp.where(most > FAST, 1, 0)
    small = [
        pltpu.make_async_copy(src, dst, small_sem.at[i])
        for i, (src, dst) in enumerate(
            ((loss_ref, loss_hbm), (adv_ref, adv_hbm), (more_ref, more_hbm))
        )
    ]
    for copy in small:
        copy.start()
    position = sliced_position(cols)
    last = members - 1
    tail[0:chunk, :] = main[last * chunk : (last + 1) * chunk, :]
    to_scalars.wait()

    def out_copy(k):
        part = pl.ds(pl.multiple_of(k * width, width), width)
        return pltpu.make_async_copy(grad.at[part], grad_hbm.at[part], out_sem.at[k])

    def one_member(k, ref, base):
        slope = numbers[2, 0, 0]
        at = base + META
        for r in range(per_dest):
            length = numbers[0, k, r].astype(jnp.int32)
            u = ref[pl.ds(at, cols), :]
            y = jnp.where(position < length, numbers[1, k, r] + slope * u, 0.0)
            first = k * width + r // 8 * (8 * cols) + r % 8
            grad[pl.ds(first, cols, stride=8), :] = y
            at = jnp.minimum(at + ((length + (LANES - 1)) >> 7), base + chunk)
        out_copy(k).start()

    @pl.loop(0, last)
    def _(k):
        one_member(k, main, pl.multiple_of(k * chunk, 8))

    one_member(last, tail, 0)

    for copy in small:
        copy.wait()

    @pl.loop(0, members)
    def _(k):
        out_copy(k).wait()


def score(main, scales, per_dest, cols):
    members, chunk, _ = main.shape
    full = per_dest * cols
    hbm = pl.BlockSpec(memory_space=pl.ANY)
    vmem = pl.BlockSpec(memory_space=pltpu.VMEM)

    def body(*refs):
        score_kernel(members, per_dest, cols, scales, refs)

    small = jax.ShapeDtypeStruct((members, per_dest), jnp.float32)
    return pl.pallas_call(
        body,
        out_shape=(
            jax.ShapeDtypeStruct((members * full, LANES), jnp.float32),
            small,
            small,
            jax.ShapeDtypeStruct((3, members, LANES), jnp.float32),
            jax.ShapeDtypeStruct((1, LANES), jnp.int32),
        ),
        in_specs=[vmem],
        out_specs=(hbm, hbm, hbm, vmem, hbm),
        scratch_shapes=[
            pltpu.VMEM((chunk + cols, LANES), jnp.float32),
            pltpu.VMEM((members * full, LANES), jnp.float32),
            pltpu.SMEM((3, members, LANES), jnp.float32),
            pltpu.VMEM((members, per_dest), jnp.float32),
            pltpu.VMEM((members, per_dest), jnp.float32),
            pltpu.VMEM((1, LANES), jnp.int32),
            pltpu.SemaphoreType.DMA,
            pltpu.SemaphoreType.DMA((members,)),
            pltpu.SemaphoreType.DMA((3,)),
        ],
        compiler_params=pltpu.CompilerParams(vmem_limit_bytes=24 << 20),
        name="score",
    )(main.reshape(members * chunk, LANES))


def finish_kernel(members, per_dest, cols, refs):
    table_hbm, rest_hbm, _, grad_hbm, numbers, rest, grad, sem = refs
    width = per_dest * cols
    spare = width - FAST
    load = pltpu.make_async_copy(table_hbm, numbers, sem.at[0])
    load.start()
    load.wait()
    position = sliced_position(cols)
    row_of = lax.broadcasted_iota(jnp.int32, (cols, LANES), 0)

    @pl.loop(0, members)
    def _(k):
        place = grad_hbm.at[pl.ds(k * width, width)]
        loads = (
            pltpu.make_async_copy(rest_hbm.at[k], rest.at[pl.ds(cols, spare)], sem.at[0]),
            pltpu.make_async_copy(place, grad, sem.at[1]),
        )
        for load in loads:
            load.start()
        for load in loads:
            load.wait()

        def row(r, at):
            length = numbers[0, k, r].astype(jnp.int32)
            end = at + ((length + (LANES - 1)) >> 7)

            @pl.when(end > FAST)
            def _():
                u = rest[pl.ds(at - FAST + cols, cols), :]
                y = jnp.where(position < length, numbers[1, k, r] + numbers[2, 0, 0] * u, 0.0)
                first = (r >> 3) * (8 * cols) + (r & 7)
                old = grad[pl.ds(first, cols, stride=8), :]
                grad[pl.ds(first, cols, stride=8), :] = jnp.where(row_of + at >= FAST, y, old)

            return end

        lax.fori_loop(0, per_dest, row, jnp.int32(0))
        store = pltpu.make_async_copy(grad, place, sem.at[1])
        store.start()
        store.wait()


def finish(grad, rest, table, per_dest, cols):
    members = rest.shape[0]
    full = per_dest * cols
    hbm = pl.BlockSpec(memory_space=pl.ANY)

    def body(*refs):
        finish_kernel(members, per_dest, cols, refs)

    return pl.pallas_call(
        body,
        out_shape=jax.ShapeDtypeStruct(grad.shape, jnp.float32),
        in_specs=[hbm, hbm, hbm],
        out_specs=hbm,
        input_output_aliases={2: 0},
        scratch_shapes=[
            pltpu.SMEM((3, members, LANES), jnp.float32),
            pltpu.VMEM((full - FAST + 2 * cols, LANES), jnp.float32),
            pltpu.VMEM((full, LANES), jnp.float32),
            pltpu.SemaphoreType.DMA((2,)),
        ],
        compiler_params=pltpu.CompilerParams(vmem_limit_bytes=8 << 20),
        name="finish",
    )(table, rest, grad)


def partner(x, step):
    size = lax.axis_size(GX)
    return lax.ppermute(x, GX, [(i, i ^ step) for i in range(size)])


def body(policy_logp, anchor_logp, lengths, rewards, slot_prompt):
    members_dev, slots, seq_slots = policy_logp.shape
    dests = lax.axis_size(GY)
    per_dest = slots // dests
    cols = seq_slots // LANES
    members = members_dev * dests
    samples = members * slots * lax.axis_size(GX)
    scales = (float(samples * seq_slots), float(samples))
    near = [lengths] + [partner(lengths, step) for step in (5, 4, 1)]
    u, sums, slot_of = token_terms(
        *(
            pltpu.with_memory_space_constraint(x, pltpu.HBM)
            for x in (lengths, rewards, slot_prompt, policy_logp[0], anchor_logp[0])
        ),
        dests,
    )
    near = added(near, slot_of)
    main, head = pack(slot_of, lengths, u, sums, dests)
    main = stamp(head, [near, partner(near, 2)], main, per_dest)
    main = lax.all_to_all(main, GY, 0, 0, tiled=True)
    grad, loss, advantage, table, more = score(main, scales, per_dest, cols)

    def the_rest(state):
        grad, _ = state
        rest = pack_rest(slot_of, lengths, u, dests)
        got = lax.all_to_all(rest, GY, 0, 0, tiled=True)
        return finish(grad, got, table, per_dest, cols), jnp.int32(0)

    grad, _ = lax.while_loop(lambda state: state[1] > 0, the_rest, (grad, more[0, 0]))
    grad = (
        grad.reshape(members, per_dest // 8, cols, 8, LANES)
        .transpose(0, 1, 3, 2, 4)
        .reshape(members, per_dest, seq_slots)
    )
    return grad, loss, advantage


def solution(mesh):
    torus = Mesh(mesh.devices.reshape(4, 2, 4, 4), ("gx_0", "gx_1", "gy_0", "gy_1"))
    return jax.shard_map(
        body,
        mesh=torus,
        in_specs=(P(GY, GX, None), P(GY, GX, None), P(GY, GX), P(GY, GX), P(GY, GX)),
        out_specs=(P(None, GX_GY, None), P(None, GX_GY), P(None, GX_GY)),
        check_vma=False,
    )
```

```python
import jax
import jax.numpy as jnp
from jax import lax
from jax.experimental import pallas as pl
from jax.experimental.pallas import tpu as pltpu
from jax.sharding import Mesh
from jax.sharding import PartitionSpec as P

GX_GY = ("gx_0", "gx_1", "gy_0", "gy_1")
GY = ("gy_0", "gy_1")
GX = ("gx_0", "gx_1")

KL = 0.1
LANES = 128
META = 8
FAST = 432


def sliced_position(cols):
    row = lax.broadcasted_iota(jnp.int32, (cols, LANES), 0)
    return row * LANES + lax.broadcasted_iota(jnp.int32, (cols, LANES), 1)


LEAST = 512
SPAN = LANES // 4
LEN, SUM_P, REWARD, SUM_Q = (i * SPAN for i in range(4))
STEPS = 16


def token_kernel(
    dests,
    small_hbm,
    policy_hbm,
    anchor_hbm,
    u_ref,
    sums_ref,
    slot_hbm,
    policy,
    anchor,
    parts,
    len_ref,
    reward_ref,
    prompt_ref,
    slot_of,
    sem,
    small_sem,
):
    slots, width = policy.shape
    rows = slots // STEPS
    cols = width // LANES
    per_dest = slots // dests

    def loads(step):
        part = pl.ds(pl.multiple_of(step * rows, rows), rows)
        return (
            pltpu.make_async_copy(policy_hbm.at[part], policy.at[part], sem.at[0, step]),
            pltpu.make_async_copy(anchor_hbm.at[part], anchor.at[part], sem.at[1, step]),
        )

    small = [
        pltpu.make_async_copy(src, dst, small_sem.at[i])
        for i, (src, dst) in enumerate(zip(small_hbm, (prompt_ref, len_ref, reward_ref)))
    ]
    for load in small:
        load.start()
    for step in range(STEPS):
        for load in loads(step):
            load.start()
    for load in small:
        load.wait()

    def invert(s, carry):
        slot_of[0, prompt_ref[0, s] & (slots - 1)] = s
        return carry

    lax.fori_loop(0, slots, invert, 0, unroll=16)
    inverse = pltpu.make_async_copy(slot_of, slot_hbm, small_sem.at[3])
    inverse.start()
    lane = lax.broadcasted_iota(jnp.int32, (8, LANES), 1)
    sub = lax.broadcasted_iota(jnp.int32, (8, LANES), 0)

    @pl.loop(0, STEPS)
    def _(step):
        for load in loads(step):
            load.wait()

        @pl.loop(0, rows // 8, unroll=2)
        def _(group):
            first = pl.multiple_of(step * rows + group * 8, 8)
            length = jnp.full((8, LANES), len_ref[0, first], jnp.int32)
            reward = jnp.full((8, LANES), reward_ref[0, first], jnp.int32)
            for i in range(1, 8):
                length = jnp.where(sub == i, len_ref[0, first + i], length)
                reward = jnp.where(sub == i, reward_ref[0, first + i], reward)
            sums_ref[pl.ds(first, 8), :] = jnp.where(lane < REWARD, length, reward).astype(
                jnp.float32
            )
            behind = lane - length
            sums_p = [jnp.zeros((8, LANES), jnp.float32)] * 4
            sums_q = [jnp.zeros((8, LANES), jnp.float32)] * 4
            for c in range(cols):
                at = (pl.ds(first, 8), pl.ds(c * LANES, LANES))
                a = policy[at]
                d = anchor[at] - a
                u = jnp.exp(d) - 1.0
                u_ref[pl.ds(first * cols + c // 8 * 64 + c % 8, 8, stride=8), :] = u
                q = u - d
                if (c + 1) * LANES > LEAST:
                    valid = behind < -c * LANES
                    q = jnp.where(valid, q, 0.0)
                    a = jnp.where(valid, a, 0.0)
                sums_q[c % 4] = sums_q[c % 4] + q
                sums_p[c % 4] = sums_p[c % 4] + a
            parts[0, pl.ds(first, 8), :] = (sums_p[0] + sums_p[1]) + (sums_p[2] + sums_p[3])
            parts[1, pl.ds(first, 8), :] = (sums_q[0] + sums_q[1]) + (sums_q[2] + sums_q[3])

    inverse.wait()
    lane = lax.broadcasted_iota(jnp.int32, (slots, LANES), 1)
    p, q = (x + pltpu.roll(x, 2 * SPAN, 1) for x in (parts[0], parts[1]))
    both = jnp.where(lane < REWARD, p, q)
    both = both + pltpu.roll(both, SPAN, 1)
    summed = (lane >= SUM_P) & (lane < REWARD) | (lane >= SUM_Q)
    sums_ref[...] = jnp.where(summed, both, sums_ref[...])


def token_terms(lengths, rewards, prompts, policy, anchor, dests):
    slots, width = policy.shape
    vmem = pl.BlockSpec(memory_space=pltpu.VMEM)
    hbm = pl.BlockSpec(memory_space=pl.ANY)

    def body(*refs):
        token_kernel(dests, refs[:3], *refs[3:])

    return pl.pallas_call(
        body,
        out_shape=(
            jax.ShapeDtypeStruct((slots * width // LANES, LANES), jnp.float32),
            jax.ShapeDtypeStruct((slots, LANES), jnp.float32),
            jax.ShapeDtypeStruct((1, slots), jnp.int32),
        ),
        in_specs=[hbm] * 5,
        out_specs=(vmem, vmem, hbm),
        scratch_shapes=[
            pltpu.VMEM((slots, width), jnp.float32),
            pltpu.VMEM((slots, width), jnp.float32),
            pltpu.VMEM((2, slots, LANES), jnp.float32),
            pltpu.SMEM((1, slots), jnp.int32),
            pltpu.SMEM((1, slots), jnp.int32),
            pltpu.SMEM((1, slots), jnp.int32),
            pltpu.SMEM((1, slots), jnp.int32),
            pltpu.SemaphoreType.DMA((2, STEPS)),
            pltpu.SemaphoreType.DMA((4,)),
        ],
        compiler_params=pltpu.CompilerParams(vmem_limit_bytes=24 << 20),
        cost_estimate=pl.CostEstimate(
            flops=40_000_000, bytes_accessed=12 * slots * width, transcendentals=slots * width
        ),
        name="token_terms",
    )(prompts, lengths, rewards, policy, anchor)


def pack_kernel(
    dests,
    per_dest,
    cols,
    slot_of,
    len_ref,
    u_ref,
    sums_ref,
    main,
    head_ref,
    stage,
    in_order,
):
    slots = dests * per_dest
    chunk = META + FAST
    last = dests - 1

    def one_dest(dest, most, ref, base):
        def row(r, at):
            p = dest * per_dest + r
            s = slot_of[0, p]
            first = pl.multiple_of((s >> 3) * (8 * cols) + (s & 7) * 8, 8)
            for j in range(cols // 8):
                ref[pl.ds(at + 8 * j, 8), :] = u_ref[pl.ds(first + 64 * j, 8), :]
            in_order[pl.ds(p, 1), :] = sums_ref[pl.ds(s, 1), :]
            return at + ((len_ref[0, s] + (LANES - 1)) >> 7)

        end = lax.fori_loop(0, per_dest, row, base + META, unroll=4)
        return jnp.maximum(most, end - base - META)

    def in_place(dest, most):
        return one_dest(dest, most, main, pl.multiple_of(dest * chunk, 8))

    most = lax.fori_loop(0, last, in_place, jnp.int32(0))
    most = one_dest(last, most, stage, 0)
    main[last * chunk + META : (last + 1) * chunk, :] = stage[META:chunk, :]

    sub = lax.broadcasted_iota(jnp.int32, (8, LANES), 0)
    lane = lax.broadcasted_iota(jnp.int32, (8, LANES), 1)
    pick = jnp.where((sub == 0) & (lane == LEN), 1.0, 0.0)
    pick = jnp.where((sub == 1) & (lane == REWARD), 0.25, pick)
    pick = jnp.where((sub == 2) & (lane >= SUM_P) & (lane < REWARD), 1.0, pick)
    pick = jnp.where((sub == 3) & (lane >= SUM_Q), 1.0, pick)
    head = lax.dot_general(
        pick,
        in_order[...],
        (((1,), (1,)), ((), ())),
        precision=lax.Precision.HIGHEST,
        preferred_element_type=jnp.float32,
    )
    sub = lax.broadcasted_iota(jnp.int32, (8, slots), 0)
    head_ref[...] = jnp.where(sub == 5, most.astype(jnp.float32), head)


def stamp_kernel(dests, per_dest, head, counts, _, main, tile, sem):
    sub = lax.broadcasted_iota(jnp.int32, (8, LANES), 0)
    count = jnp.sum(sum(c[...] for c in counts).astype(jnp.float32), axis=1, keepdims=True)
    halves = head.shape[1] // LANES
    for half in range(halves):
        tile[half] = jnp.where(sub == 4, count, head[:, half * LANES : (half + 1) * LANES])
    copies = [
        pltpu.make_async_copy(
            tile.at[dest * per_dest // LANES], main.at[dest, pl.ds(0, META)], sem.at[dest]
        )
        for dest in range(dests)
    ]
    for copy in copies:
        copy.start()
    for copy in copies:
        copy.wait()


def stamp(head, counts, main, per_dest):
    dests = main.shape[0]
    vmem = pl.BlockSpec(memory_space=pltpu.VMEM)
    place = pl.BlockSpec(memory_space=pl.ANY)

    def body(head, *refs):
        stamp_kernel(dests, per_dest, head, refs[: len(counts)], *refs[len(counts) :])

    return pl.pallas_call(
        body,
        out_shape=jax.ShapeDtypeStruct(main.shape, jnp.float32),
        in_specs=[vmem] * (1 + len(counts)) + [place],
        out_specs=place,
        input_output_aliases={1 + len(counts): 0},
        scratch_shapes=[
            pltpu.VMEM((head.shape[1] // LANES, META, LANES), jnp.float32),
            pltpu.SemaphoreType.DMA((dests,)),
        ],
        compiler_params=pltpu.CompilerParams(vmem_limit_bytes=4 << 20),
        name="stamp",
    )(head, *counts, main)


def added(parts, after):
    def body(*refs):
        refs[-1][...] = sum(x[...] for x in refs[:-2])

    vmem = pl.BlockSpec(memory_space=pltpu.VMEM)
    return pl.pallas_call(
        body,
        out_shape=jax.ShapeDtypeStruct(parts[0].shape, parts[0].dtype),
        in_specs=[vmem] * len(parts) + [pl.BlockSpec(memory_space=pl.ANY)],
        out_specs=vmem,
        compiler_params=pltpu.CompilerParams(vmem_limit_bytes=4 << 20),
        name="added",
    )(*parts, after)


def pack(slot_of, lengths, u, sums, dests):
    slots = lengths.shape[1]
    per_dest = slots // dests
    cols = u.shape[0] // slots
    chunk = META + FAST
    smem = pl.BlockSpec(memory_space=pltpu.SMEM)
    vmem = pl.BlockSpec(memory_space=pltpu.VMEM)

    def body(*refs):
        pack_kernel(dests, per_dest, cols, *refs)

    main, head = pl.pallas_call(
        body,
        out_shape=(
            jax.ShapeDtypeStruct((dests * chunk, LANES), jnp.float32),
            jax.ShapeDtypeStruct((META, slots), jnp.float32),
        ),
        in_specs=[smem] * 2 + [vmem] * 2,
        out_specs=(vmem, vmem),
        scratch_shapes=[
            pltpu.VMEM((META + (per_dest + 1) * cols, LANES), jnp.float32),
            pltpu.VMEM((slots, LANES), jnp.float32),
        ],
        compiler_params=pltpu.CompilerParams(vmem_limit_bytes=24 << 20),
        cost_estimate=pl.CostEstimate(
            flops=40_000_000, bytes_accessed=8 * dests * chunk * LANES, transcendentals=0
        ),
        name="pack",
    )(slot_of, lengths, u, sums)
    return main.reshape(dests, chunk, LANES), head


def pack_rest(slot_of, lengths, u, dests):
    slots = lengths.shape[1]
    per_dest = slots // dests
    cols = u.shape[0] // slots
    spare = per_dest * cols - FAST

    def body(slot_of, len_ref, u_ref, rest_hbm, stage, sem):
        @pl.loop(0, dests)
        def _(dest):
            def row(r, at):
                s = slot_of[0, dest * per_dest + r]
                first = pl.multiple_of((s >> 3) * (8 * cols) + (s & 7) * 8, 8)
                for j in range(cols // 8):
                    stage[pl.ds(at + 8 * j, 8), :] = u_ref[pl.ds(first + 64 * j, 8), :]
                return at + ((len_ref[0, s] + (LANES - 1)) >> 7)

            lax.fori_loop(0, per_dest, row, jnp.int32(0))
            copy = pltpu.make_async_copy(stage.at[pl.ds(FAST, spare)], rest_hbm.at[dest], sem)
            copy.start()
            copy.wait()

    smem = pl.BlockSpec(memory_space=pltpu.SMEM)
    return pl.pallas_call(
        body,
        out_shape=jax.ShapeDtypeStruct((dests, spare, LANES), jnp.float32),
        in_specs=[smem, smem, pl.BlockSpec(memory_space=pltpu.VMEM)],
        out_specs=pl.BlockSpec(memory_space=pl.ANY),
        scratch_shapes=[
            pltpu.VMEM(((per_dest + 1) * cols, LANES), jnp.float32),
            pltpu.SemaphoreType.DMA,
        ],
        compiler_params=pltpu.CompilerParams(vmem_limit_bytes=16 << 20),
        name="pack_rest",
    )(slot_of, lengths, u)


def score_kernel(members, per_dest, cols, scales, refs):
    (
        main,
        grad_hbm,
        loss_hbm,
        adv_hbm,
        table_ref,
        more_hbm,
        tail,
        grad,
        numbers,
        loss_ref,
        adv_ref,
        more_ref,
        num_sem,
        out_sem,
        small_sem,
    ) = refs
    grad_scale, loss_scale = scales
    width = per_dest * cols
    chunk = META + FAST

    def field(i):
        return jnp.concatenate(
            [main[k * chunk + i : k * chunk + i + 1, :] for k in range(members)], axis=0
        )

    start = lax.rem(lax.axis_index(GY) * per_dest, LANES)
    shift = lax.rem(LANES - start, LANES)
    lengths, reward, sums_p, sums_q = (pltpu.roll(field(i), shift, 1) for i in range(4))
    total = jnp.sum(reward, axis=0, keepdims=True)
    advantage = (members * reward - total) / (members - 1)
    tokens = jnp.sum(field(4), axis=0, keepdims=True)
    scale = grad_scale / tokens
    table_ref[0] = lengths
    table_ref[1] = -advantage * scale
    table_ref[2] = jnp.broadcast_to(scale * -KL, (members, LANES))
    to_scalars = pltpu.make_async_copy(table_ref, numbers, num_sem)
    to_scalars.start()
    loss = (KL * sums_q - advantage * sums_p) * (loss_scale / tokens)
    loss_ref[...] = loss[:, 0:per_dest]
    adv_ref[...] = advantage[:, 0:per_dest]
    most = jnp.max(field(5), axis=0, keepdims=True)
    more_ref[...] = jnp.where(most > FAST, 1, 0)
    small = [
        pltpu.make_async_copy(src, dst, small_sem.at[i])
        for i, (src, dst) in enumerate(
            ((loss_ref, loss_hbm), (adv_ref, adv_hbm), (more_ref, more_hbm))
        )
    ]
    for copy in small:
        copy.start()
    position = sliced_position(cols)
    last = members - 1
    tail[0:chunk, :] = main[last * chunk : (last + 1) * chunk, :]
    to_scalars.wait()

    def out_copy(k):
        part = pl.ds(pl.multiple_of(k * width, width), width)
        return pltpu.make_async_copy(grad.at[part], grad_hbm.at[part], out_sem.at[k])

    def one_member(k, ref, base):
        slope = numbers[2, 0, 0]
        at = base + META
        for r in range(per_dest):
            length = numbers[0, k, r].astype(jnp.int32)
            u = ref[pl.ds(at, cols), :]
            y = jnp.where(position < length, numbers[1, k, r] + slope * u, 0.0)
            first = k * width + r // 8 * (8 * cols) + r % 8
            grad[pl.ds(first, cols, stride=8), :] = y
            at = jnp.minimum(at + ((length + (LANES - 1)) >> 7), base + chunk)
        out_copy(k).start()

    @pl.loop(0, last)
    def _(k):
        one_member(k, main, pl.multiple_of(k * chunk, 8))

    one_member(last, tail, 0)

    for copy in small:
        copy.wait()

    @pl.loop(0, members)
    def _(k):
        out_copy(k).wait()


def score(main, scales, per_dest, cols):
    members, chunk, _ = main.shape
    full = per_dest * cols
    hbm = pl.BlockSpec(memory_space=pl.ANY)
    vmem = pl.BlockSpec(memory_space=pltpu.VMEM)

    def body(*refs):
        score_kernel(members, per_dest, cols, scales, refs)

    small = jax.ShapeDtypeStruct((members, per_dest), jnp.float32)
    return pl.pallas_call(
        body,
        out_shape=(
            jax.ShapeDtypeStruct((members * full, LANES), jnp.float32),
            small,
            small,
            jax.ShapeDtypeStruct((3, members, LANES), jnp.float32),
            jax.ShapeDtypeStruct((1, LANES), jnp.int32),
        ),
        in_specs=[vmem],
        out_specs=(hbm, hbm, hbm, vmem, hbm),
        scratch_shapes=[
            pltpu.VMEM((chunk + cols, LANES), jnp.float32),
            pltpu.VMEM((members * full, LANES), jnp.float32),
            pltpu.SMEM((3, members, LANES), jnp.float32),
            pltpu.VMEM((members, per_dest), jnp.float32),
            pltpu.VMEM((members, per_dest), jnp.float32),
            pltpu.VMEM((1, LANES), jnp.int32),
            pltpu.SemaphoreType.DMA,
            pltpu.SemaphoreType.DMA((members,)),
            pltpu.SemaphoreType.DMA((3,)),
        ],
        compiler_params=pltpu.CompilerParams(vmem_limit_bytes=24 << 20),
        name="score",
    )(main.reshape(members * chunk, LANES))


def finish_kernel(members, per_dest, cols, refs):
    table_hbm, rest_hbm, _, grad_hbm, numbers, rest, grad, sem = refs
    width = per_dest * cols
    spare = width - FAST
    load = pltpu.make_async_copy(table_hbm, numbers, sem.at[0])
    load.start()
    load.wait()
    position = sliced_position(cols)
    row_of = lax.broadcasted_iota(jnp.int32, (cols, LANES), 0)

    @pl.loop(0, members)
    def _(k):
        place = grad_hbm.at[pl.ds(k * width, width)]
        loads = (
            pltpu.make_async_copy(rest_hbm.at[k], rest.at[pl.ds(cols, spare)], sem.at[0]),
            pltpu.make_async_copy(place, grad, sem.at[1]),
        )
        for load in loads:
            load.start()
        for load in loads:
            load.wait()

        def row(r, at):
            length = numbers[0, k, r].astype(jnp.int32)
            end = at + ((length + (LANES - 1)) >> 7)

            @pl.when(end > FAST)
            def _():
                u = rest[pl.ds(at - FAST + cols, cols), :]
                y = jnp.where(position < length, numbers[1, k, r] + numbers[2, 0, 0] * u, 0.0)
                first = (r >> 3) * (8 * cols) + (r & 7)
                old = grad[pl.ds(first, cols, stride=8), :]
                grad[pl.ds(first, cols, stride=8), :] = jnp.where(row_of + at >= FAST, y, old)

            return end

        lax.fori_loop(0, per_dest, row, jnp.int32(0))
        store = pltpu.make_async_copy(grad, place, sem.at[1])
        store.start()
        store.wait()


def finish(grad, rest, table, per_dest, cols):
    members = rest.shape[0]
    full = per_dest * cols
    hbm = pl.BlockSpec(memory_space=pl.ANY)

    def body(*refs):
        finish_kernel(members, per_dest, cols, refs)

    return pl.pallas_call(
        body,
        out_shape=jax.ShapeDtypeStruct(grad.shape, jnp.float32),
        in_specs=[hbm, hbm, hbm],
        out_specs=hbm,
        input_output_aliases={2: 0},
        scratch_shapes=[
            pltpu.SMEM((3, members, LANES), jnp.float32),
            pltpu.VMEM((full - FAST + 2 * cols, LANES), jnp.float32),
            pltpu.VMEM((full, LANES), jnp.float32),
            pltpu.SemaphoreType.DMA((2,)),
        ],
        compiler_params=pltpu.CompilerParams(vmem_limit_bytes=8 << 20),
        name="finish",
    )(table, rest, grad)


def partner(x, step):
    size = lax.axis_size(GX)
    return lax.ppermute(x, GX, [(i, i ^ step) for i in range(size)])


def body(policy_logp, anchor_logp, lengths, rewards, slot_prompt):
    members_dev, slots, seq_slots = policy_logp.shape
    dests = lax.axis_size(GY)
    per_dest = slots // dests
    cols = seq_slots // LANES
    members = members_dev * dests
    samples = members * slots * lax.axis_size(GX)
    scales = (float(samples * seq_slots), float(samples))
    near = [lengths] + [partner(lengths, step) for step in (5, 4, 1)]
    u, sums, slot_of = token_terms(
        *(
            pltpu.with_memory_space_constraint(x, pltpu.HBM)
            for x in (lengths, rewards, slot_prompt, policy_logp[0], anchor_logp[0])
        ),
        dests,
    )
    near = added(near, slot_of)
    main, head = pack(slot_of, lengths, u, sums, dests)
    main = stamp(head, [near, partner(near, 2)], main, per_dest)
    main = lax.all_to_all(main, GY, 0, 0, tiled=True)
    grad, loss, advantage, table, more = score(main, scales, per_dest, cols)

    def the_rest(state):
        grad, _ = state
        rest = pack_rest(slot_of, lengths, u, dests)
        got = lax.all_to_all(rest, GY, 0, 0, tiled=True)
        return finish(grad, got, table, per_dest, cols), jnp.int32(0)

    grad, _ = lax.while_loop(lambda state: state[1] > 0, the_rest, (grad, more[0, 0]))
    grad = (
        grad.reshape(members, per_dest // 8, cols, 8, LANES)
        .transpose(0, 1, 3, 2, 4)
        .reshape(members, per_dest, seq_slots)
    )
    return grad, loss, advantage


def solution(mesh):
    torus = Mesh(mesh.devices.reshape(4, 2, 4, 4), ("gx_0", "gx_1", "gy_0", "gy_1"))
    return jax.shard_map(
        body,
        mesh=torus,
        in_specs=(P(GY, GX, None), P(GY, GX, None), P(GY, GX), P(GY, GX), P(GY, GX)),
        out_specs=(P(None, GX_GY, None), P(None, GX_GY), P(None, GX_GY)),
        check_vma=False,
    )
```
